32 devices in a mesh: tm: 16 (over z, y, core), asset: 2 (over x).
Axes of the slice: x: 2, y: 2, z: 4, core: 2. Of those that a mesh axis runs over, the one named last changes fastest.
Arguments:
- tick_bars: float32 [2, 16, 61440], P('asset', 'tm'), may hold values from -20 to 20
- prior_bars: float32 [2, 16, 6400], P('asset', 'tm'), may hold values from -20 to 20, as said below
Outputs:
- connectedness: float32 [48, 8192], P('tm', 'asset')
The draws below stay inside these ranges and needn't reach their ends.
Inputs may be any that keep to these rules, and one draw needn't show every extreme that they name: `prior_bars`: bar returns of the same assets.
All inputs are finite; a program needn't handle non-finite values.
Results may differ from the reference program's by a relative error of at most 0.0014.
Values may be sent and summed in bfloat16 or wider, within the bound.
A program may use at most 64 MiB of HBM per device.

```python
import math
import jax
import jax.numpy as jnp
from jax import lax

ASSETS = 8192
SPAN = 30
STRIDE = 5
LEAD = 25
BARS = 240
WINDOWS = 48
N_TM = 16


cluster_count = 16


def return_draw(key, count, salt):
    tile_cols = ASSETS // 2
    log_scale = jax.random.uniform(jax.random.fold_in(key, 11), (2, 1, tile_cols), jnp.float32, math.log(0.1), math.log(3.0))
    scales = jnp.exp(log_scale)
    first_pick = jax.random.randint(jax.random.fold_in(key, 13), (2, tile_cols), 0, cluster_count)
    second_pick = jax.random.randint(jax.random.fold_in(key, 14), (2, tile_cols), 0, cluster_count)
    cluster = jnp.minimum(first_pick, second_pick)
    signs = 2.0 * jax.random.randint(jax.random.fold_in(key, 15), (2, 1, tile_cols), 0, 2).astype(jnp.float32) - 1.0
    loading = signs * jax.random.uniform(jax.random.fold_in(key, 16), (2, 1, tile_cols), jnp.float32, 0.3, 1.3)
    noise_key = jax.random.fold_in(key, salt)
    sector_moves = jnp.clip(jax.random.normal(jax.random.fold_in(noise_key, 3), (count, cluster_count), jnp.float32), -3.0, 3.0)
    sector_vol = jnp.exp(jax.random.uniform(jax.random.fold_in(noise_key, 4), (count, cluster_count), jnp.float32, math.log(0.4), math.log(2.0)))
    sector_factor = sector_moves * sector_vol
    asset_factor = jnp.transpose(sector_factor[:, cluster], (1, 0, 2))
    idiosyncratic = jnp.clip(jax.random.normal(noise_key, (2, count, tile_cols), jnp.float32), -4.0, 4.0)
    drawn = scales * (loading * asset_factor + idiosyncratic)
    drawn = jnp.clip(drawn, -19.5, 19.5)
    group_cols = ASSETS // (2 * N_TM)
    grid = drawn.reshape(2, count, N_TM, group_cols)
    return jnp.transpose(grid, (0, 2, 1, 3)).reshape(2, N_TM, count * group_cols).astype(jnp.float32)


def draw_tick_bars(key, part):
    return return_draw(key, BARS, 21)


def draw_prior_bars(key, part):
    return return_draw(key, LEAD, 22)


def setup_inputs(seed: int = 0) -> dict:
    streams_of = jax.random.split(jax.random.key(seed), 3)
    return {
        "tick_bars": draw_tick_bars(jax.random.fold_in(streams_of[2], 71), 0),
        "prior_bars": draw_prior_bars(jax.random.fold_in(streams_of[2], 71), 0),
    }


FLOOR_SQUARES = 1.0

def standardize(values):
    centred = values - lax.optimization_barrier(jnp.mean(values, axis=0, keepdims=True))
    squares = lax.optimization_barrier(jnp.sum(centred * centred, axis=0, keepdims=True))
    return (centred * lax.rsqrt(jnp.maximum(squares, FLOOR_SQUARES))).astype(jnp.bfloat16)

def unfold(packed, count):
    group_cols = ASSETS // (2 * N_TM)
    grid = packed.reshape(2, N_TM, count, group_cols)
    return jnp.transpose(grid, (2, 0, 1, 3)).reshape(count, ASSETS)

def reference(tick_bars, prior_bars):
    series_now = unfold(tick_bars, BARS)
    series_prior = unfold(prior_bars, LEAD)
    series = jnp.concatenate([series_prior, series_now], axis=0)
    block_rows = min(2048, ASSETS)

    def one_window(window_index):
        values = lax.dynamic_slice_in_dim(series, window_index * STRIDE, SPAN, 0)
        scaled = standardize(values).astype(jnp.float32)
        pieces = []
        for offset in range(0, ASSETS, block_rows):
            correlation = jnp.dot(scaled[:, offset:offset + block_rows].T, scaled, preferred_element_type=jnp.float32)
            magnitude = jnp.abs(correlation.astype(jnp.bfloat16)).astype(jnp.float32)
            pieces.append(lax.optimization_barrier(jnp.sum(magnitude, axis=1)))
        return jnp.concatenate(pieces) * (math.sqrt(SPAN) / ASSETS)
    return lax.map(one_window, jnp.arange(WINDOWS, dtype=jnp.int32))
```

```python
import functools
import math

import jax
import jax.numpy as jnp
from jax import lax
from jax.experimental import pallas as pl
from jax.experimental.pallas import tpu as pltpu
from jax.sharding import PartitionSpec as P

ASSETS = 8192
SPAN = 30
STRIDE = 5
WIN_DEV = 3
LEAD = 25
DEPTH = 32
TILE = 256
LANES = 128
SUBLANES = 8
CHUNK = 4
PART_SCALE = 256.0


FLOOR_SQUARES = 1.0


def cycle_next(time, tile):
    core = time % 2
    along = (1 + core + tile) % 2
    return time + along * (1 - 2 * core), tile + (1 - along) * (1 - 2 * tile)


def around(block, forward):
    times, tiles = lax.axis_size("tm"), lax.axis_size("asset")
    route = []
    for time in range(times):
        for tile in range(tiles):
            next_time, next_tile = cycle_next(time, tile)
            hop = (time * tiles + tile, next_time * tiles + next_tile)
            route.append(hop if forward else hop[::-1])
    return lax.ppermute(block, ("tm", "asset"), route)


def window_stack(extended):
    columns = extended.shape[1]
    count = (extended.shape[0] - SPAN) // STRIDE + 1
    groups = extended.reshape(-1, STRIDE, columns)
    stacked = jnp.stack(
        [groups[offset : offset + count] for offset in range(SPAN // STRIDE)], axis=1
    )
    values = stacked.reshape(count, SPAN, columns)
    centred = values - jnp.mean(values, axis=1, keepdims=True)
    squares = jnp.sum(centred * centred, axis=1, keepdims=True)
    scaled = (centred * lax.rsqrt(jnp.maximum(squares, FLOOR_SQUARES))).astype(jnp.bfloat16)
    return jnp.pad(scaled, ((0, 0), (0, DEPTH - SPAN), (0, 0)))


def split_parts(block):
    scaled = block.astype(jnp.float32) * PART_SCALE
    high = scaled.astype(jnp.float8_e4m3fn).astype(jnp.float32)
    return high, scaled - high


def right_parts(block):
    high, low = split_parts(block)
    return jnp.concatenate([high, high, low, low], axis=0).astype(jnp.float8_e4m3fn)


def strip_totals(rows, source, first, count, column_sums, own_first):
    groups, _, width = source.shape
    high, low = split_parts(rows)
    rows_t = jnp.concatenate([high, low, high, low], axis=0).T.astype(jnp.float8_e4m3fn)
    row_partial = jnp.zeros((width, LANES), jnp.float32)
    for offset in range(count):
        group = lax.rem(first + offset, groups)
        magnitude = jnp.abs(jnp.dot(rows_t, source[group], preferred_element_type=jnp.float32))
        for lane in range(0, width, LANES):
            row_partial = row_partial + magnitude[:, lane : lane + LANES]
        if offset or not own_first:
            folded = jnp.sum(magnitude.reshape(width // SUBLANES, SUBLANES, width), axis=0)
            column_sums[group] = column_sums[group] + folded
    return jnp.sum(row_partial.T, axis=0, keepdims=True)


def fill_parts(source, parts):
    def fill(group, carry):
        parts[group] = right_parts(source[group])
        return carry

    lax.fori_loop(0, source.shape[0], fill, 0)


def diagonal(source, out, column_sums, parts):
    groups = source.shape[0]
    half = groups // 2
    fill_parts(source, parts)
    column_sums[...] = jnp.zeros_like(column_sums)

    def step(index, carry):
        out[index, 0] = strip_totals(source[index], parts, index, half + 1, column_sums, True)
        later = index + half
        out[later, 0] = strip_totals(source[later], parts, later, half, column_sums, True)
        return carry

    lax.fori_loop(0, half, step, 0)
    out[:, 0] = out[:, 0] + jnp.sum(column_sums[...], axis=1, keepdims=True)


def totals_kernel(crosses, own, other, own_out, other_out, column_sums, parts):
    groups = own.shape[0]

    @pl.when(crosses[0] == 1)
    def _():
        fill_parts(other, parts)
        column_sums[...] = jnp.zeros_like(column_sums)

        def step(index, carry):
            own_out[index, 0] = strip_totals(own[index], parts, 0, groups, column_sums, False)
            return carry

        lax.fori_loop(0, groups, step, 0)
        other_out[:, 0] = jnp.sum(column_sums[...], axis=1, keepdims=True)

    @pl.when(crosses[0] == 0)
    def _():
        diagonal(own, own_out, column_sums, parts)
        diagonal(other, other_out, column_sums, parts)


def pair_totals(crosses, own, other):
    groups, depth, width = own.shape
    block = pl.BlockSpec((groups, DEPTH, width), lambda w, *_: (0, w, 0))
    line = pl.BlockSpec((groups, 1, 1, width), lambda w, *_: (0, w, 0, 0))
    return pl.pallas_call(
        totals_kernel,
        out_shape=[jax.ShapeDtypeStruct((groups, depth // DEPTH, 1, width), jnp.float32)] * 2,
        grid_spec=pltpu.PrefetchScalarGridSpec(
            num_scalar_prefetch=1,
            grid=(depth // DEPTH,),
            in_specs=[block, block],
            out_specs=[line, line],
            scratch_shapes=[
                pltpu.VMEM((groups, SUBLANES, width), jnp.float32),
                pltpu.VMEM((groups, 4 * DEPTH, width), jnp.float8_e4m3fn),
            ],
        ),
    )(crosses, own, other)


def windows_kernel(tick, prior, out, series):
    width = series.shape[1]
    lead = prior.shape[1] // width
    for row in range(lead):
        series[row : row + 1] = prior[:, row * width : (row + 1) * width]
    for row in range(tick.shape[1] // width):
        series[lead + row : lead + row + 1] = tick[:, row * width : (row + 1) * width]
    for window in range(out.shape[0] * WIN_DEV):
        values = series[window * STRIDE : window * STRIDE + SPAN]
        centred = values - jnp.sum(values, axis=0, keepdims=True) * (1.0 / SPAN)
        squares = jnp.sum(centred * centred, axis=0, keepdims=True)
        scaled = centred * lax.rsqrt(jnp.maximum(squares, FLOOR_SQUARES))
        scaled = jnp.concatenate([scaled, jnp.zeros((DEPTH - SPAN, width), jnp.float32)], axis=0)
        first = window % WIN_DEV * DEPTH
        out[window // WIN_DEV, first : first + DEPTH] = scaled.astype(jnp.bfloat16)


def deliver_kernel(groups, outgoing, own, other, own_send, own_recv, next_send, next_recv, local_sem):
    time = lax.axis_index("tm")
    tile = lax.axis_index("asset")
    next_time, next_tile = cycle_next(time, tile)
    barrier = pltpu.get_barrier_semaphore()
    for step in range(1, groups):
        peer = lax.rem(time + step, groups)
        pl.semaphore_signal(
            barrier, inc=1, device_id=(peer, tile), device_id_type=pl.DeviceIdType.MESH
        )
    pl.semaphore_signal(
        barrier, inc=1, device_id=(time, 1 - tile), device_id_type=pl.DeviceIdType.MESH
    )
    pl.semaphore_wait(barrier, groups)

    def send(step):
        peer = lax.rem(time + step, groups)
        return pltpu.make_async_remote_copy(
            src_ref=outgoing.at[peer],
            dst_ref=own.at[time],
            send_sem=own_send.at[step],
            recv_sem=own_recv.at[step],
            device_id=(peer, tile),
            device_id_type=pl.DeviceIdType.MESH,
        )

    def forward(step):
        source = lax.rem(time - step + groups, groups)
        return pltpu.make_async_remote_copy(
            src_ref=own.at[source],
            dst_ref=other.at[source],
            send_sem=next_send.at[source],
            recv_sem=next_recv.at[source],
            device_id=(next_time, next_tile),
            device_id_type=pl.DeviceIdType.MESH,
        )

    sends = [send(step) for step in range(1, groups)]
    for copy in sends:
        copy.start()
    local = pltpu.make_async_copy(outgoing.at[time], own.at[time], local_sem)
    local.start()
    local.wait()
    forwards = [forward(step) for step in range(groups)]
    forwards[0].start()
    for step in range(1, groups):
        sends[step - 1].wait_recv()
        forwards[step].start()
    for copy in sends:
        copy.wait_send()
    for group in range(groups):
        arrival = pltpu.make_async_remote_copy(
            src_ref=own.at[group],
            dst_ref=other.at[group],
            send_sem=next_send.at[group],
            recv_sem=next_recv.at[group],
            device_id=(next_time, next_tile),
            device_id_type=pl.DeviceIdType.MESH,
        )
        arrival.wait()


def delivered(outgoing):
    groups = outgoing.shape[0]
    vmem = pl.BlockSpec(memory_space=pltpu.VMEM)
    return pl.pallas_call(
        functools.partial(deliver_kernel, groups),
        out_shape=[jax.ShapeDtypeStruct(outgoing.shape, outgoing.dtype)] * 2,
        in_specs=[vmem],
        out_specs=[vmem, vmem],
        scratch_shapes=[pltpu.SemaphoreType.DMA((groups,))] * 4 + [pltpu.SemaphoreType.DMA],
        compiler_params=pltpu.CompilerParams(collective_id=0, has_side_effects=True),
    )(outgoing)


def local_windows(tick_bars, prior_bars):
    groups = lax.axis_size("tm")
    width = ASSETS // (2 * groups)
    ticks, prior = tick_bars.reshape(1, -1), prior_bars.reshape(1, -1)
    if width % LANES:
        series = jnp.concatenate([prior.reshape(-1, width), ticks.reshape(-1, width)], axis=0)
        return window_stack(series).reshape(groups, WIN_DEV * DEPTH, width)
    rows = (ticks.size + prior.size) // width
    return pl.pallas_call(
        windows_kernel,
        out_shape=jax.ShapeDtypeStruct((groups, WIN_DEV * DEPTH, width), jnp.bfloat16),
        scratch_shapes=[pltpu.VMEM((-(-rows // SUBLANES) * SUBLANES, width), jnp.float32)],
    )(ticks, prior)


def retiled(blocks):
    groups, depth, width = blocks.shape
    if width % LANES == 0:
        return blocks
    join = TILE // width
    grouped = blocks.reshape(groups // join, join, depth, width)
    return jnp.transpose(grouped, (0, 2, 1, 3)).reshape(groups // join, depth, TILE)


def tree(terms):
    terms = list(terms)
    while len(terms) > 1:
        paired = [terms[k] + terms[k + 1] for k in range(0, len(terms) - 1, 2)]
        terms = paired + terms[len(paired) * 2 :]
    return terms[0]


def magnitudes(lhs, rhs):
    correlation = jnp.dot(lhs, rhs, preferred_element_type=jnp.float32)
    return jnp.abs(correlation.astype(jnp.bfloat16))


def lane_folded(block):
    return tree(block[:, k : k + LANES] for k in range(0, block.shape[1], LANES))


def sublane_folded(block, rows):
    return tree(block[k : k + rows] for k in range(0, block.shape[0], rows))


def add_rows(totals, partial):
    totals[...] = totals[...] + sublane_folded(partial.astype(jnp.float32).T, SUBLANES)


def add_columns(totals, partials):
    pairs = [tree(partials[k : k + 2]).astype(jnp.float32) for k in range(0, len(partials), 2)]
    totals[...] = totals[...] + sublane_folded(tree(pairs), SUBLANES)


def cross_unit(left, right, row_totals, column_totals):
    columns = [[] for _ in range(CHUNK)]
    for u in range(CHUNK):
        lhs, folded = left[u], []
        for o in range(CHUNK):
            block = magnitudes(lhs, right[o])
            folded.append(lane_folded(block))
            columns[o].append(sublane_folded(block, 2 * SUBLANES))
        add_rows(row_totals.at[u], tree(folded))
    for o in range(CHUNK):
        add_columns(column_totals.at[o], columns[o])


def diagonal_unit(left, right, totals):
    columns = [[] for _ in range(CHUNK)]
    for u in range(CHUNK):
        lhs, folded = left[u], []
        for o in range(u, CHUNK):
            block = magnitudes(lhs, right[o])
            folded.append(lane_folded(block))
            if o > u:
                columns[o].append(sublane_folded(block, 2 * SUBLANES))
        add_rows(totals.at[u], tree(folded))
    for o in range(1, CHUNK):
        add_columns(totals.at[o], columns[o])


def prepare(series, left, right, window):
    halves = []
    for half in range(2):
        values = series[half, STRIDE * window : STRIDE * window + SPAN]
        centred = values - jnp.sum(values, axis=0, keepdims=True) * (1.0 / SPAN)
        squares = jnp.sum(centred * centred, axis=0, keepdims=True)
        scaled = centred * lax.rsqrt(jnp.maximum(squares, FLOOR_SQUARES))
        halves.append(scaled.astype(jnp.bfloat16))
    scaled = jnp.concatenate(halves, axis=1).astype(jnp.float32)
    pad = jnp.zeros((DEPTH - SPAN, scaled.shape[1]), jnp.float32)
    high, low = split_parts(jnp.concatenate([scaled, pad], axis=0))
    high, low = high.astype(jnp.float8_e4m3fn), low.astype(jnp.float8_e4m3fn)
    right[...] = jnp.concatenate([high, high, low, low], axis=0)
    left[...] = jnp.concatenate([high, low, high, low], axis=0).T


def partner(index, step, size):
    bit, mirrored = 1, index
    while bit < size:
        if step // bit % 2:
            mirrored = mirrored + bit - 2 * bit * (mirrored // bit % 2)
        bit *= 2
    return mirrored


def connect_kernel(
    groups, tick, prior, out, ticks, priors, outgoing, own, other, left, right, totals, sums, back,
    load_sem, own_send, own_recv, next_send, next_recv, back_send, back_recv,
):
    width = 2 * LANES
    blocks = groups // CHUNK
    time, tile = lax.axis_index("tm"), lax.axis_index("asset")
    core = time % 2
    crosses = 1 - (core + tile) % 2
    next_time, next_tile = cycle_next(time, tile)
    along = (1 + core + tile) % 2
    prev_time, prev_tile = time + (1 - along) * (1 - 2 * core), tile + along * (1 - 2 * tile)
    block, place = time // CHUNK, time % CHUNK
    loads = [
        pltpu.make_async_copy(prior, priors, load_sem.at[0]),
        pltpu.make_async_copy(tick, ticks, load_sem.at[1]),
    ]
    for load in loads:
        load.start()
    barrier = pltpu.get_barrier_semaphore()
    steps = [(s, r) for s in range(blocks) for r in range(CHUNK)]

    def peer(s, r):
        return partner(block, s, blocks) * CHUNK + partner(place, r, CHUNK)

    for s, r in steps[1:]:
        pl.semaphore_signal(
            barrier, inc=1, device_id=(peer(s, r), tile), device_id_type=pl.DeviceIdType.MESH
        )
    pl.semaphore_signal(
        barrier, inc=1, device_id=(time, 1 - tile), device_id_type=pl.DeviceIdType.MESH
    )
    for load in loads:
        load.wait()
    bars = WIN_DEV * STRIDE
    for owner in range(groups):
        first = owner * bars - LEAD
        early = min(max(-first, 0), bars + LEAD)
        for half in range(2):
            if early:
                begin = 2 * (LEAD - early) + half
                outgoing[owner, half, :early] = priors[pl.ds(begin, early, stride=2), :]
            begin = 2 * (first + early) + half
            late = bars + LEAD - early
            outgoing[owner, half, early:] = ticks[pl.ds(begin, late, stride=2), :]
    pl.semaphore_wait(barrier, groups)

    def send(s, r):
        index = s * CHUNK + r
        return pltpu.make_async_remote_copy(
            src_ref=outgoing.at[peer(s, r)],
            dst_ref=own.at[index],
            send_sem=own_send.at[index],
            recv_sem=own_recv.at[index],
            device_id=(peer(s, r), tile),
            device_id_type=pl.DeviceIdType.MESH,
        )

    def forward(s, r):
        index = s * CHUNK + r
        return pltpu.make_async_remote_copy(
            src_ref=own.at[index],
            dst_ref=other.at[index],
            send_sem=next_send.at[index],
            recv_sem=next_recv.at[index],
            device_id=(next_time, next_tile),
            device_id_type=pl.DeviceIdType.MESH,
        )

    local = pltpu.make_async_copy(outgoing.at[time], own.at[0], load_sem.at[0])
    local.start()
    sends = {step: send(*step) for step in steps[1:]}
    for step in steps[1:]:
        sends[step].start()
    forwards = {step: forward(*step) for step in steps}

    totals[...] = jnp.zeros_like(totals)

    def pass_on(s):
        for r in range(CHUNK):
            if s or r:
                sends[s, r].wait_recv()
            else:
                local.wait()
            forwards[s, r].start()

    def units(s):
        for r in range(CHUNK):
            forwards[s, r].wait_recv()

        def fill(i, carry):
            group = s * CHUNK + i
            for window in range(WIN_DEV):
                prepare(own.at[group], left.at[0, window, group], right.at[0, window, group], window)
                prepare(other.at[group], left.at[1, window, group], right.at[1, window, group], window)
            return carry

        lax.fori_loop(0, CHUNK, fill, 0)

        def chunk_of(ref, which, window, k):
            return ref.at[which, window, pl.ds(k * CHUNK, CHUNK)]

        def pair(k, carry):
            for window in range(WIN_DEV):
                for side in range(2):
                    row_set, column_set = (1 - crosses, 1) if side else (0, crosses)
                    row_chunk, column_chunk = (k, s) if side else (s, k)
                    cross_unit(
                        chunk_of(left, row_set, window, row_chunk),
                        chunk_of(right, column_set, window, column_chunk),
                        chunk_of(totals, row_set, window, row_chunk),
                        chunk_of(totals, column_set, window, column_chunk),
                    )
            return carry

        lax.fori_loop(0, s, pair, 0)

        @pl.when(crosses == 1)
        def _():
            for window in range(WIN_DEV):
                cross_unit(
                    chunk_of(left, 0, window, s),
                    chunk_of(right, 1, window, s),
                    chunk_of(totals, 0, window, s),
                    chunk_of(totals, 1, window, s),
                )

        @pl.when(crosses == 0)
        def _():
            for window in range(WIN_DEV):
                for which in range(2):
                    diagonal_unit(
                        chunk_of(left, which, window, s),
                        chunk_of(right, which, window, s),
                        chunk_of(totals, which, window, s),
                    )

    pass_on(0)
    pass_on(1)
    units(0)
    pass_on(2)
    units(1)
    pass_on(3)
    units(2)
    units(3)

    sums[...] = jnp.sum(totals[1], axis=2, keepdims=True)
    returned = pltpu.make_async_remote_copy(
        src_ref=sums,
        dst_ref=back,
        send_sem=back_send,
        recv_sem=back_recv,
        device_id=(prev_time, prev_tile),
        device_id_type=pl.DeviceIdType.MESH,
    )
    returned.start()
    for step in steps[1:]:
        sends[step].wait_send()
    for step in steps:
        forwards[step].wait_send()
    mine = jnp.sum(totals[0], axis=2, keepdims=True)
    returned.wait()
    scale = math.sqrt(SPAN) / (ASSETS * PART_SCALE * PART_SCALE)
    mine = (mine + back[...]) * scale
    for s, r in steps:
        lanes = pl.ds(pl.multiple_of(peer(s, r) * width, LANES), width)
        for window in range(WIN_DEV):
            out[window : window + 1, lanes] = mine[window, s * CHUNK + r]


def connected(tick_bars, prior_bars):
    groups = lax.axis_size("tm")
    ticks, prior = tick_bars.reshape(-1, LANES), prior_bars.reshape(-1, LANES)
    width = 2 * LANES
    block = (groups, 2, WIN_DEV * STRIDE + LEAD, LANES)
    dma = pltpu.SemaphoreType.DMA
    f8 = jnp.float8_e4m3fn
    return pl.pallas_call(
        functools.partial(connect_kernel, groups),
        out_shape=jax.ShapeDtypeStruct((WIN_DEV, groups * width), jnp.float32),
        in_specs=[pl.BlockSpec(memory_space=pl.ANY)] * 2,
        out_specs=pl.BlockSpec(memory_space=pltpu.VMEM),
        scratch_shapes=[
            pltpu.VMEM(ticks.shape, jnp.float32),
            pltpu.VMEM(prior.shape, jnp.float32),
            pltpu.VMEM(block, jnp.float32),
            pltpu.VMEM(block, jnp.float32),
            pltpu.VMEM(block, jnp.float32),
            pltpu.VMEM((2, WIN_DEV, groups, width, 4 * DEPTH), f8),
            pltpu.VMEM((2, WIN_DEV, groups, 4 * DEPTH, width), f8),
            pltpu.VMEM((2, WIN_DEV, groups, SUBLANES, width), jnp.float32),
            pltpu.VMEM((WIN_DEV, groups, 1, width), jnp.float32),
            pltpu.VMEM((WIN_DEV, groups, 1, width), jnp.float32),
            dma((2,)), dma((groups,)), dma((groups,)), dma((groups,)), dma((groups,)), dma, dma,
        ],
        compiler_params=pltpu.CompilerParams(
            collective_id=1, has_side_effects=True, vmem_limit_bytes=60 * 1024 * 1024
        ),
    )(ticks, prior)


def shards(tick_bars, prior_bars):
    groups = lax.axis_size("tm")
    if groups == 4 * CHUNK and ASSETS == groups * 4 * LANES:
        return connected(tick_bars, prior_bars)
    own, other = delivered(local_windows(tick_bars, prior_bars))
    own, other = retiled(own), retiled(other)
    core = lax.axis_index("tm") % 2
    crosses = (core == lax.axis_index("asset")).astype(jnp.int32).reshape(1)
    own_part, other_part = pair_totals(crosses, own, other)
    own_part = jnp.transpose(own_part[:, :, 0], (1, 0, 2)).reshape(WIN_DEV, -1)
    other_part = jnp.transpose(other_part[:, :, 0], (1, 0, 2)).reshape(WIN_DEV, -1)
    returned = around(other_part, False)
    return (own_part + returned) * (math.sqrt(SPAN) / (ASSETS * PART_SCALE * PART_SCALE))


def solution(mesh):
    in_specs = (P("asset", "tm", None), P("asset", "tm", None))
    out_specs = P("tm", "asset")
    return jax.shard_map(shards, mesh=mesh, in_specs=in_specs, out_specs=out_specs, check_vma=False)
```

```python
import functools
import math

import jax
import jax.numpy as jnp
from jax import lax
from jax.experimental import pallas as pl
from jax.experimental.pallas import tpu as pltpu
from jax.sharding import PartitionSpec as P

ASSETS = 8192
SPAN = 30
STRIDE = 5
WIN_DEV = 3
LEAD = 25
DEPTH = 32
TILE = 256
LANES = 128
SUBLANES = 8
CHUNK = 4
UNIT = 16
PART_SCALE = 256.0


FLOOR_SQUARES = 1.0


def cycle_next(time, tile):
    core = time % 2
    along = (1 + core + tile) % 2
    return time + along * (1 - 2 * core), tile + (1 - along) * (1 - 2 * tile)


def around(block, forward):
    times, tiles = lax.axis_size("tm"), lax.axis_size("asset")
    route = []
    for time in range(times):
        for tile in range(tiles):
            next_time, next_tile = cycle_next(time, tile)
            hop = (time * tiles + tile, next_time * tiles + next_tile)
            route.append(hop if forward else hop[::-1])
    return lax.ppermute(block, ("tm", "asset"), route)


def window_stack(extended):
    columns = extended.shape[1]
    count = (extended.shape[0] - SPAN) // STRIDE + 1
    groups = extended.reshape(-1, STRIDE, columns)
    stacked = jnp.stack(
        [groups[offset : offset + count] for offset in range(SPAN // STRIDE)], axis=1
    )
    values = stacked.reshape(count, SPAN, columns)
    centred = values - jnp.mean(values, axis=1, keepdims=True)
    squares = jnp.sum(centred * centred, axis=1, keepdims=True)
    scaled = (centred * lax.rsqrt(jnp.maximum(squares, FLOOR_SQUARES))).astype(jnp.bfloat16)
    return jnp.pad(scaled, ((0, 0), (0, DEPTH - SPAN), (0, 0)))


def split_parts(block):
    scaled = block.astype(jnp.float32) * PART_SCALE
    high = scaled.astype(jnp.float8_e4m3fn).astype(jnp.float32)
    return high, scaled - high


def right_parts(block):
    high, low = split_parts(block)
    return jnp.concatenate([high, high, low, low], axis=0).astype(jnp.float8_e4m3fn)


def strip_totals(rows, source, first, count, column_sums, own_first):
    groups, _, width = source.shape
    high, low = split_parts(rows)
    rows_t = jnp.concatenate([high, low, high, low], axis=0).T.astype(jnp.float8_e4m3fn)
    row_partial = jnp.zeros((width, LANES), jnp.float32)
    for offset in range(count):
        group = lax.rem(first + offset, groups)
        magnitude = jnp.abs(jnp.dot(rows_t, source[group], preferred_element_type=jnp.float32))
        for lane in range(0, width, LANES):
            row_partial = row_partial + magnitude[:, lane : lane + LANES]
        if offset or not own_first:
            folded = jnp.sum(magnitude.reshape(width // SUBLANES, SUBLANES, width), axis=0)
            column_sums[group] = column_sums[group] + folded
    return jnp.sum(row_partial.T, axis=0, keepdims=True)


def fill_parts(source, parts):
    def fill(group, carry):
        parts[group] = right_parts(source[group])
        return carry

    lax.fori_loop(0, source.shape[0], fill, 0)


def diagonal(source, out, column_sums, parts):
    groups = source.shape[0]
    half = groups // 2
    fill_parts(source, parts)
    column_sums[...] = jnp.zeros_like(column_sums)

    def step(index, carry):
        out[index, 0] = strip_totals(source[index], parts, index, half + 1, column_sums, True)
        later = index + half
        out[later, 0] = strip_totals(source[later], parts, later, half, column_sums, True)
        return carry

    lax.fori_loop(0, half, step, 0)
    out[:, 0] = out[:, 0] + jnp.sum(column_sums[...], axis=1, keepdims=True)


def totals_kernel(crosses, own, other, own_out, other_out, column_sums, parts):
    groups = own.shape[0]

    @pl.when(crosses[0] == 1)
    def _():
        fill_parts(other, parts)
        column_sums[...] = jnp.zeros_like(column_sums)

        def step(index, carry):
            own_out[index, 0] = strip_totals(own[index], parts, 0, groups, column_sums, False)
            return carry

        lax.fori_loop(0, groups, step, 0)
        other_out[:, 0] = jnp.sum(column_sums[...], axis=1, keepdims=True)

    @pl.when(crosses[0] == 0)
    def _():
        diagonal(own, own_out, column_sums, parts)
        diagonal(other, other_out, column_sums, parts)


def pair_totals(crosses, own, other):
    groups, depth, width = own.shape
    block = pl.BlockSpec((groups, DEPTH, width), lambda w, *_: (0, w, 0))
    line = pl.BlockSpec((groups, 1, 1, width), lambda w, *_: (0, w, 0, 0))
    return pl.pallas_call(
        totals_kernel,
        out_shape=[jax.ShapeDtypeStruct((groups, depth // DEPTH, 1, width), jnp.float32)] * 2,
        grid_spec=pltpu.PrefetchScalarGridSpec(
            num_scalar_prefetch=1,
            grid=(depth // DEPTH,),
            in_specs=[block, block],
            out_specs=[line, line],
            scratch_shapes=[
                pltpu.VMEM((groups, SUBLANES, width), jnp.float32),
                pltpu.VMEM((groups, 4 * DEPTH, width), jnp.float8_e4m3fn),
            ],
        ),
    )(crosses, own, other)


def windows_kernel(tick, prior, out, series):
    width = series.shape[1]
    lead = prior.shape[1] // width
    for row in range(lead):
        series[row : row + 1] = prior[:, row * width : (row + 1) * width]
    for row in range(tick.shape[1] // width):
        series[lead + row : lead + row + 1] = tick[:, row * width : (row + 1) * width]
    for window in range(out.shape[0] * WIN_DEV):
        values = series[window * STRIDE : window * STRIDE + SPAN]
        centred = values - jnp.sum(values, axis=0, keepdims=True) * (1.0 / SPAN)
        squares = jnp.sum(centred * centred, axis=0, keepdims=True)
        scaled = centred * lax.rsqrt(jnp.maximum(squares, FLOOR_SQUARES))
        scaled = jnp.concatenate([scaled, jnp.zeros((DEPTH - SPAN, width), jnp.float32)], axis=0)
        first = window % WIN_DEV * DEPTH
        out[window // WIN_DEV, first : first + DEPTH] = scaled.astype(jnp.bfloat16)


def deliver_kernel(groups, outgoing, own, other, own_send, own_recv, next_send, next_recv, local_sem):
    time = lax.axis_index("tm")
    tile = lax.axis_index("asset")
    next_time, next_tile = cycle_next(time, tile)
    barrier = pltpu.get_barrier_semaphore()
    for step in range(1, groups):
        peer = lax.rem(time + step, groups)
        pl.semaphore_signal(
            barrier, inc=1, device_id=(peer, tile), device_id_type=pl.DeviceIdType.MESH
        )
    pl.semaphore_signal(
        barrier, inc=1, device_id=(time, 1 - tile), device_id_type=pl.DeviceIdType.MESH
    )
    pl.semaphore_wait(barrier, groups)

    def send(step):
        peer = lax.rem(time + step, groups)
        return pltpu.make_async_remote_copy(
            src_ref=outgoing.at[peer],
            dst_ref=own.at[time],
            send_sem=own_send.at[step],
            recv_sem=own_recv.at[step],
            device_id=(peer, tile),
            device_id_type=pl.DeviceIdType.MESH,
        )

    def forward(step):
        source = lax.rem(time - step + groups, groups)
        return pltpu.make_async_remote_copy(
            src_ref=own.at[source],
            dst_ref=other.at[source],
            send_sem=next_send.at[source],
            recv_sem=next_recv.at[source],
            device_id=(next_time, next_tile),
            device_id_type=pl.DeviceIdType.MESH,
        )

    sends = [send(step) for step in range(1, groups)]
    for copy in sends:
        copy.start()
    local = pltpu.make_async_copy(outgoing.at[time], own.at[time], local_sem)
    local.start()
    local.wait()
    forwards = [forward(step) for step in range(groups)]
    forwards[0].start()
    for step in range(1, groups):
        sends[step - 1].wait_recv()
        forwards[step].start()
    for copy in sends:
        copy.wait_send()
    for group in range(groups):
        arrival = pltpu.make_async_remote_copy(
            src_ref=own.at[group],
            dst_ref=other.at[group],
            send_sem=next_send.at[group],
            recv_sem=next_recv.at[group],
            device_id=(next_time, next_tile),
            device_id_type=pl.DeviceIdType.MESH,
        )
        arrival.wait()


def delivered(outgoing):
    groups = outgoing.shape[0]
    vmem = pl.BlockSpec(memory_space=pltpu.VMEM)
    return pl.pallas_call(
        functools.partial(deliver_kernel, groups),
        out_shape=[jax.ShapeDtypeStruct(outgoing.shape, outgoing.dtype)] * 2,
        in_specs=[vmem],
        out_specs=[vmem, vmem],
        scratch_shapes=[pltpu.SemaphoreType.DMA((groups,))] * 4 + [pltpu.SemaphoreType.DMA],
        compiler_params=pltpu.CompilerParams(collective_id=0, has_side_effects=True),
    )(outgoing)


def local_windows(tick_bars, prior_bars):
    groups = lax.axis_size("tm")
    width = ASSETS // (2 * groups)
    ticks, prior = tick_bars.reshape(1, -1), prior_bars.reshape(1, -1)
    if width % LANES:
        series = jnp.concatenate([prior.reshape(-1, width), ticks.reshape(-1, width)], axis=0)
        return window_stack(series).reshape(groups, WIN_DEV * DEPTH, width)
    rows = (ticks.size + prior.size) // width
    return pl.pallas_call(
        windows_kernel,
        out_shape=jax.ShapeDtypeStruct((groups, WIN_DEV * DEPTH, width), jnp.bfloat16),
        scratch_shapes=[pltpu.VMEM((-(-rows // SUBLANES) * SUBLANES, width), jnp.float32)],
    )(ticks, prior)


def retiled(blocks):
    groups, depth, width = blocks.shape
    if width % LANES == 0:
        return blocks
    join = TILE // width
    grouped = blocks.reshape(groups // join, join, depth, width)
    return jnp.transpose(grouped, (0, 2, 1, 3)).reshape(groups // join, depth, TILE)


def tree(terms):
    terms = list(terms)
    while len(terms) > 1:
        paired = [terms[k] + terms[k + 1] for k in range(0, len(terms) - 1, 2)]
        terms = paired + terms[len(paired) * 2 :]
    return terms[0]


def magnitudes(lhs, rhs):
    correlation = jnp.dot(lhs, rhs, preferred_element_type=jnp.float32)
    return jnp.abs(correlation.astype(jnp.bfloat16))


def lane_folded(block):
    return tree(block[:, k : k + LANES] for k in range(0, block.shape[1], LANES))


def sublane_folded(block, rows):
    return tree(block[k : k + rows] for k in range(0, block.shape[0], rows))


def add_rows(totals, partial):
    folded = sublane_folded(partial.T, LANES // 4)
    totals[...] = totals[...] + sublane_folded(folded.astype(jnp.float32), SUBLANES)


def add_columns(totals, partials):
    partial = tree(partials).astype(jnp.float32)
    totals[...] = totals[...] + sublane_folded(partial, SUBLANES)


def unit_totals(left, right, row_totals, column_totals, diagonal):
    columns = [[] for _ in range(CHUNK)]
    for u in range(CHUNK):
        lhs, folded = left[u], []
        for o in range(u if diagonal else 0, CHUNK):
            block = magnitudes(lhs, right[o])
            folded.append(lane_folded(block))
            if diagonal and o == u:
                continue
            columns[o].append(sublane_folded(block, 2 * SUBLANES))
            if len(columns[o]) == 2 or u == CHUNK - 1 or (diagonal and u == o - 1):
                add_columns(column_totals.at[o], columns[o])
                columns[o] = []
        add_rows(row_totals.at[u], tree(folded))


def prepare(series, left, right, window):
    halves = []
    shape = (DEPTH, LANES)
    bar = lax.broadcasted_iota(jnp.int32, shape, 0) + STRIDE * window
    held = (bar != UNIT - 1) & (bar != 2 * UNIT - 1)
    for half in range(2):
        values = series[half, STRIDE * window : STRIDE * window + DEPTH]
        mean = jnp.sum(values, axis=0, keepdims=True) * (1.0 / SPAN)
        centred = jnp.where(held, values - mean, 0.0)
        squares = jnp.sum(centred * centred, axis=0, keepdims=True)
        scaled = centred * lax.rsqrt(jnp.maximum(squares, FLOOR_SQUARES))
        halves.append(scaled.astype(jnp.bfloat16))
    high, low = split_parts(jnp.concatenate(halves, axis=1))
    high, low = high.astype(jnp.float8_e4m3fn), low.astype(jnp.float8_e4m3fn)
    right[...] = jnp.concatenate([high, high, low, low], axis=0)
    left[...] = jnp.concatenate([high, low, high, low], axis=0).T


def lay_out(ticks, priors, series):
    bars = WIN_DEV * STRIDE
    total = LEAD + ticks.shape[0] // 2
    for unit in range(series.shape[1] // UNIT):
        first = unit * bars
        early = min(max(LEAD - first, 0), bars)
        late = min(total - first, bars) - early
        for half in range(2):
            for bar in range(early):
                lane = (2 * (first + bar) + half) * LANES
                row = unit * UNIT + bar
                series[half, row : row + 1] = priors[:, lane : lane + LANES]
            row, end = unit * UNIT + early, (unit + 1) * UNIT
            filled = [jnp.zeros((end - row - late, LANES), jnp.float32)]
            if late:
                begin = 2 * (first + early - LEAD) + half
                filled.insert(0, ticks[pl.ds(begin, late, stride=2), :])
            series[half, row:end] = jnp.concatenate(filled, axis=0)


def partner(index, step, size):
    bit, mirrored = 1, index
    while bit < size:
        if step // bit % 2:
            mirrored = mirrored + bit - 2 * bit * (mirrored // bit % 2)
        bit *= 2
    return mirrored


def connect_kernel(
    groups, tick, prior, out, ticks, priors, series, along_block, own, other, left, right,
    totals, sums, back, load_sem, block_send, block_recv, own_send, own_recv,
    next_send, next_recv, back_send, back_recv,
):
    width = 2 * LANES
    blocks = groups // CHUNK
    time, tile = lax.axis_index("tm"), lax.axis_index("asset")
    core = time % 2
    along = (1 + core + tile) % 2
    crosses = along
    next_time, next_tile = cycle_next(time, tile)
    prev_time, prev_tile = time + (1 - along) * (1 - 2 * core), tile + along * (1 - 2 * tile)
    block, place = time // CHUNK, time % CHUNK

    loads = [
        pltpu.make_async_copy(prior, priors, load_sem.at[0]),
        pltpu.make_async_copy(tick, ticks, load_sem.at[1]),
    ]
    for load in loads:
        load.start()
    barrier = pltpu.get_barrier_semaphore()

    def block_at(s):
        return partner(block, s, blocks)

    def place_at(r):
        return partner(place, r, CHUNK)

    peers = [(block_at(s) * CHUNK + place, tile) for s in range(1, blocks)]
    peers += [(block * CHUNK + place_at(r), tile) for r in range(1, CHUNK)]
    peers += [(time, 1 - tile)]
    for peer in peers:
        pl.semaphore_signal(barrier, inc=1, device_id=peer, device_id_type=pl.DeviceIdType.MESH)
    for load in loads:
        load.wait()
    lay_out(ticks, priors, series)
    pl.semaphore_wait(barrier, len(peers))

    reach = own.shape[2]
    block_rows = CHUNK * UNIT

    def remote(source, target, sent, received, device):
        return pltpu.make_async_remote_copy(
            src_ref=source,
            dst_ref=target,
            send_sem=sent,
            recv_sem=received,
            device_id=device,
            device_id_type=pl.DeviceIdType.MESH,
        )

    def part(s, spot):
        if s:
            return along_block.at[s, :, pl.ds(pl.multiple_of(spot * UNIT, UNIT), reach)]
        return series.at[:, pl.ds(pl.multiple_of(block * block_rows + spot * UNIT, UNIT), reach)]

    def block_copy(s):
        first = pl.multiple_of(block_at(s) * block_rows, UNIT)
        return remote(
            series.at[:, pl.ds(first, along_block.shape[2])],
            along_block.at[s],
            block_send.at[s],
            block_recv.at[s],
            (block_at(s) * CHUNK + place, tile),
        )

    def place_copy(s, r):
        index = s * CHUNK + r
        return remote(
            part(s, place_at(r)),
            own.at[index],
            own_send.at[index],
            own_recv.at[index],
            (block * CHUNK + place_at(r), tile),
        )

    def held_part(s, r):
        return own.at[s * CHUNK + r] if r else part(s, place)

    def next_copy(s, r):
        index = s * CHUNK + r
        return remote(
            held_part(s, r),
            other.at[index],
            next_send.at[index],
            next_recv.at[index],
            (next_time, next_tile),
        )

    steps = [(s, r) for s in range(blocks) for r in range(CHUNK)]
    block_copies = {s: block_copy(s) for s in range(1, blocks)}
    place_copies = {(s, r): place_copy(s, r) for s, r in steps if r}
    next_copies = {step: next_copy(*step) for step in steps}

    def relay(s):
        if s:
            block_copies[s].wait_recv()
        for r in reversed(range(1, CHUNK)):
            place_copies[s, r].start()
        next_copies[s, 0].start()

    def pass_on(s):
        for r in range(1, CHUNK):
            place_copies[s, r].wait_recv()
            next_copies[s, r].start()

    def prepare_set(which, s):
        for r in range(CHUNK):
            group = s * CHUNK + r
            if which:
                next_copies[s, r].wait_recv()
            source = other.at[group] if which else held_part(s, r)
            for window in range(WIN_DEV):
                prepare(source, left.at[which, window, group], right.at[which, window, group], window)

    def chunk_of(ref, which, window, k):
        return ref.at[which, window, pl.ds(k * CHUNK, CHUNK)]

    def unit(window, row_set, row_chunk, column_set, column_chunk, diagonal=False):
        unit_totals(
            chunk_of(left, row_set, window, row_chunk),
            chunk_of(right, column_set, window, column_chunk),
            chunk_of(totals, row_set, window, row_chunk),
            chunk_of(totals, column_set, window, column_chunk),
            diagonal,
        )

    def pairs(s, first, last):
        def pair(k, carry):
            for window in range(WIN_DEV):
                unit(window, 0, s, crosses, k)
                unit(window, 1 - crosses, k, 1, s)
            return carry

        lax.fori_loop(first, last, pair, 0)

    def closing(s):
        @pl.when(crosses == 1)
        def _():
            for window in range(WIN_DEV):
                unit(window, 0, s, 1, s)

        @pl.when(crosses == 0)
        def _():
            for window in range(WIN_DEV):
                unit(window, 0, s, 0, s, True)
                unit(window, 1, s, 1, s, True)

    for s in range(1, blocks):
        block_copies[s].start()
    relay(0)
    totals[...] = jnp.zeros_like(totals)
    pass_on(0)
    relay(1)
    prepare_set(0, 0)
    prepare_set(1, 0)
    closing(0)
    pass_on(1)
    relay(2)
    prepare_set(0, 1)
    prepare_set(1, 1)
    pairs(1, 0, 1)
    pass_on(2)
    relay(3)
    closing(1)
    prepare_set(0, 2)
    prepare_set(1, 2)
    pairs(2, 0, 1)
    pass_on(3)
    pairs(2, 1, 2)
    closing(2)
    prepare_set(0, 3)
    prepare_set(1, 3)
    pairs(3, 0, 3)
    closing(3)

    sums[...] = jnp.sum(totals[1], axis=2, keepdims=True)
    returned = remote(sums, back, back_send, back_recv, (prev_time, prev_tile))
    returned.start()
    for copy in (*block_copies.values(), *place_copies.values(), *next_copies.values()):
        copy.wait_send()
    mine = jnp.sum(totals[0], axis=2, keepdims=True)
    returned.wait()
    mine = mine + back[...]
    for s, r in steps:
        first = (block_at(s) * CHUNK + place_at(r)) * width
        lanes = pl.ds(pl.multiple_of(first, LANES), width)
        for window in range(WIN_DEV):
            out[window : window + 1, lanes] = mine[window, s * CHUNK + r]


def connected(tick_bars, prior_bars):
    groups = lax.axis_size("tm")
    ticks, prior = tick_bars.reshape(-1, LANES), prior_bars.reshape(1, -1)
    width = 2 * LANES
    blocks = groups // CHUNK
    reach = -(-(WIN_DEV * STRIDE + LEAD) // (WIN_DEV * STRIDE)) * UNIT
    ahead = reach - UNIT
    shared = (groups, 2, reach, LANES)
    vmem, dma, f8 = pltpu.VMEM, pltpu.SemaphoreType.DMA, jnp.float8_e4m3fn
    raw = pl.pallas_call(
        functools.partial(connect_kernel, groups),
        out_shape=jax.ShapeDtypeStruct((WIN_DEV, groups * width), jnp.float32),
        in_specs=[pl.BlockSpec(memory_space=pl.ANY)] * 2,
        out_specs=pl.BlockSpec(memory_space=vmem),
        scratch_shapes=[
            vmem(ticks.shape, jnp.float32),
            vmem(prior.shape, jnp.float32),
            vmem((2, groups * UNIT + ahead, LANES), jnp.float32),
            vmem((blocks, 2, CHUNK * UNIT + ahead, LANES), jnp.float32),
            vmem(shared, jnp.float32),
            vmem(shared, jnp.float32),
            vmem((2, WIN_DEV, groups, width, 4 * DEPTH), f8),
            vmem((2, WIN_DEV, groups, 4 * DEPTH, width), f8),
            vmem((2, WIN_DEV, groups, SUBLANES, width), jnp.float32),
            vmem((WIN_DEV, groups, 1, width), jnp.float32),
            vmem((WIN_DEV, groups, 1, width), jnp.float32),
            dma((2,)), dma((blocks,)), dma((blocks,)), dma((groups,)), dma((groups,)),
            dma((groups,)), dma((groups,)), dma, dma,
        ],
        compiler_params=pltpu.CompilerParams(
            collective_id=1,
            has_side_effects=True,
            vmem_limit_bytes=60 * 1024 * 1024,
        ),
    )(ticks, prior)
    return raw * (math.sqrt(SPAN) / (ASSETS * PART_SCALE * PART_SCALE))


def shards(tick_bars, prior_bars):
    groups = lax.axis_size("tm")
    if groups == 4 * CHUNK and ASSETS == groups * 4 * LANES:
        return connected(tick_bars, prior_bars)
    own, other = delivered(local_windows(tick_bars, prior_bars))
    own, other = retiled(own), retiled(other)
    core = lax.axis_index("tm") % 2
    crosses = (core == lax.axis_index("asset")).astype(jnp.int32).reshape(1)
    own_part, other_part = pair_totals(crosses, own, other)
    own_part = jnp.transpose(own_part[:, :, 0], (1, 0, 2)).reshape(WIN_DEV, -1)
    other_part = jnp.transpose(other_part[:, :, 0], (1, 0, 2)).reshape(WIN_DEV, -1)
    returned = around(other_part, False)
    return (own_part + returned) * (math.sqrt(SPAN) / (ASSETS * PART_SCALE * PART_SCALE))


def solution(mesh):
    in_specs = (P("asset", "tm", None), P("asset", "tm", None))
    out_specs = P("tm", "asset")
    return jax.shard_map(shards, mesh=mesh, in_specs=in_specs, out_specs=out_specs, check_vma=False)
```

```python
import functools
import math

import jax
import jax.numpy as jnp
from jax import lax
from jax.experimental import pallas as pl
from jax.experimental.pallas import tpu as pltpu
from jax.sharding import PartitionSpec as P

ASSETS = 8192
SPAN = 30
STRIDE = 5
WIN_DEV = 3
LEAD = 25
DEPTH = 32
TILE = 256
LANES = 128
SUBLANES = 8
CHUNK = 4
UNIT = 16
PART_SCALE = 256.0


FLOOR_SQUARES = 1.0


def cycle_next(time, tile):
    core = time % 2
    along = (1 + core + tile) % 2
    return time + along * (1 - 2 * core), tile + (1 - along) * (1 - 2 * tile)


def around(block, forward):
    times, tiles = lax.axis_size("tm"), lax.axis_size("asset")
    route = []
    for time in range(times):
        for tile in range(tiles):
            next_time, next_tile = cycle_next(time, tile)
            hop = (time * tiles + tile, next_time * tiles + next_tile)
            route.append(hop if forward else hop[::-1])
    return lax.ppermute(block, ("tm", "asset"), route)


def window_stack(extended):
    columns = extended.shape[1]
    count = (extended.shape[0] - SPAN) // STRIDE + 1
    groups = extended.reshape(-1, STRIDE, columns)
    stacked = jnp.stack(
        [groups[offset : offset + count] for offset in range(SPAN // STRIDE)], axis=1
    )
    values = stacked.reshape(count, SPAN, columns)
    centred = values - jnp.mean(values, axis=1, keepdims=True)
    squares = jnp.sum(centred * centred, axis=1, keepdims=True)
    scaled = (centred * lax.rsqrt(jnp.maximum(squares, FLOOR_SQUARES))).astype(jnp.bfloat16)
    return jnp.pad(scaled, ((0, 0), (0, DEPTH - SPAN), (0, 0)))


def split_parts(block):
    scaled = block.astype(jnp.float32) * PART_SCALE
    high = scaled.astype(jnp.float8_e4m3fn).astype(jnp.float32)
    return high, scaled - high


def right_parts(block):
    high, low = split_parts(block)
    return jnp.concatenate([high, high, low, low], axis=0).astype(jnp.float8_e4m3fn)


def strip_totals(rows, source, first, count, column_sums, own_first):
    groups, _, width = source.shape
    high, low = split_parts(rows)
    rows_t = jnp.concatenate([high, low, high, low], axis=0).T.astype(jnp.float8_e4m3fn)
    row_partial = jnp.zeros((width, LANES), jnp.float32)
    for offset in range(count):
        group = lax.rem(first + offset, groups)
        magnitude = jnp.abs(jnp.dot(rows_t, source[group], preferred_element_type=jnp.float32))
        for lane in range(0, width, LANES):
            row_partial = row_partial + magnitude[:, lane : lane + LANES]
        if offset or not own_first:
            folded = jnp.sum(magnitude.reshape(width // SUBLANES, SUBLANES, width), axis=0)
            column_sums[group] = column_sums[group] + folded
    return jnp.sum(row_partial.T, axis=0, keepdims=True)


def fill_parts(source, parts):
    def fill(group, carry):
        parts[group] = right_parts(source[group])
        return carry

    lax.fori_loop(0, source.shape[0], fill, 0)


def diagonal(source, out, column_sums, parts):
    groups = source.shape[0]
    half = groups // 2
    fill_parts(source, parts)
    column_sums[...] = jnp.zeros_like(column_sums)

    def step(index, carry):
        out[index, 0] = strip_totals(source[index], parts, index, half + 1, column_sums, True)
        later = index + half
        out[later, 0] = strip_totals(source[later], parts, later, half, column_sums, True)
        return carry

    lax.fori_loop(0, half, step, 0)
    out[:, 0] = out[:, 0] + jnp.sum(column_sums[...], axis=1, keepdims=True)


def totals_kernel(crosses, own, other, own_out, other_out, column_sums, parts):
    groups = own.shape[0]

    @pl.when(crosses[0] == 1)
    def _():
        fill_parts(other, parts)
        column_sums[...] = jnp.zeros_like(column_sums)

        def step(index, carry):
            own_out[index, 0] = strip_totals(own[index], parts, 0, groups, column_sums, False)
            return carry

        lax.fori_loop(0, groups, step, 0)
        other_out[:, 0] = jnp.sum(column_sums[...], axis=1, keepdims=True)

    @pl.when(crosses[0] == 0)
    def _():
        diagonal(own, own_out, column_sums, parts)
        diagonal(other, other_out, column_sums, parts)


def pair_totals(crosses, own, other):
    groups, depth, width = own.shape
    block = pl.BlockSpec((groups, DEPTH, width), lambda w, *_: (0, w, 0))
    line = pl.BlockSpec((groups, 1, 1, width), lambda w, *_: (0, w, 0, 0))
    return pl.pallas_call(
        totals_kernel,
        out_shape=[jax.ShapeDtypeStruct((groups, depth // DEPTH, 1, width), jnp.float32)] * 2,
        grid_spec=pltpu.PrefetchScalarGridSpec(
            num_scalar_prefetch=1,
            grid=(depth // DEPTH,),
            in_specs=[block, block],
            out_specs=[line, line],
            scratch_shapes=[
                pltpu.VMEM((groups, SUBLANES, width), jnp.float32),
                pltpu.VMEM((groups, 4 * DEPTH, width), jnp.float8_e4m3fn),
            ],
        ),
    )(crosses, own, other)


def windows_kernel(tick, prior, out, series):
    width = series.shape[1]
    lead = prior.shape[1] // width
    for row in range(lead):
        series[row : row + 1] = prior[:, row * width : (row + 1) * width]
    for row in range(tick.shape[1] // width):
        series[lead + row : lead + row + 1] = tick[:, row * width : (row + 1) * width]
    for window in range(out.shape[0] * WIN_DEV):
        values = series[window * STRIDE : window * STRIDE + SPAN]
        centred = values - jnp.sum(values, axis=0, keepdims=True) * (1.0 / SPAN)
        squares = jnp.sum(centred * centred, axis=0, keepdims=True)
        scaled = centred * lax.rsqrt(jnp.maximum(squares, FLOOR_SQUARES))
        scaled = jnp.concatenate([scaled, jnp.zeros((DEPTH - SPAN, width), jnp.float32)], axis=0)
        first = window % WIN_DEV * DEPTH
        out[window // WIN_DEV, first : first + DEPTH] = scaled.astype(jnp.bfloat16)


def deliver_kernel(groups, outgoing, own, other, own_send, own_recv, next_send, next_recv, local_sem):
    time = lax.axis_index("tm")
    tile = lax.axis_index("asset")
    next_time, next_tile = cycle_next(time, tile)
    barrier = pltpu.get_barrier_semaphore()
    for step in range(1, groups):
        peer = lax.rem(time + step, groups)
        pl.semaphore_signal(
            barrier, inc=1, device_id=(peer, tile), device_id_type=pl.DeviceIdType.MESH
        )
    pl.semaphore_signal(
        barrier, inc=1, device_id=(time, 1 - tile), device_id_type=pl.DeviceIdType.MESH
    )
    pl.semaphore_wait(barrier, groups)

    def send(step):
        peer = lax.rem(time + step, groups)
        return pltpu.make_async_remote_copy(
            src_ref=outgoing.at[peer],
            dst_ref=own.at[time],
            send_sem=own_send.at[step],
            recv_sem=own_recv.at[step],
            device_id=(peer, tile),
            device_id_type=pl.DeviceIdType.MESH,
        )

    def forward(step):
        source = lax.rem(time - step + groups, groups)
        return pltpu.make_async_remote_copy(
            src_ref=own.at[source],
            dst_ref=other.at[source],
            send_sem=next_send.at[source],
            recv_sem=next_recv.at[source],
            device_id=(next_time, next_tile),
            device_id_type=pl.DeviceIdType.MESH,
        )

    sends = [send(step) for step in range(1, groups)]
    for copy in sends:
        copy.start()
    local = pltpu.make_async_copy(outgoing.at[time], own.at[time], local_sem)
    local.start()
    local.wait()
    forwards = [forward(step) for step in range(groups)]
    forwards[0].start()
    for step in range(1, groups):
        sends[step - 1].wait_recv()
        forwards[step].start()
    for copy in sends:
        copy.wait_send()
    for group in range(groups):
        arrival = pltpu.make_async_remote_copy(
            src_ref=own.at[group],
            dst_ref=other.at[group],
            send_sem=next_send.at[group],
            recv_sem=next_recv.at[group],
            device_id=(next_time, next_tile),
            device_id_type=pl.DeviceIdType.MESH,
        )
        arrival.wait()


def delivered(outgoing):
    groups = outgoing.shape[0]
    vmem = pl.BlockSpec(memory_space=pltpu.VMEM)
    return pl.pallas_call(
        functools.partial(deliver_kernel, groups),
        out_shape=[jax.ShapeDtypeStruct(outgoing.shape, outgoing.dtype)] * 2,
        in_specs=[vmem],
        out_specs=[vmem, vmem],
        scratch_shapes=[pltpu.SemaphoreType.DMA((groups,))] * 4 + [pltpu.SemaphoreType.DMA],
        compiler_params=pltpu.CompilerParams(collective_id=0, has_side_effects=True),
    )(outgoing)


def local_windows(tick_bars, prior_bars):
    groups = lax.axis_size("tm")
    width = ASSETS // (2 * groups)
    ticks, prior = tick_bars.reshape(1, -1), prior_bars.reshape(1, -1)
    if width % LANES:
        series = jnp.concatenate([prior.reshape(-1, width), ticks.reshape(-1, width)], axis=0)
        return window_stack(series).reshape(groups, WIN_DEV * DEPTH, width)
    rows = (ticks.size + prior.size) // width
    return pl.pallas_call(
        windows_kernel,
        out_shape=jax.ShapeDtypeStruct((groups, WIN_DEV * DEPTH, width), jnp.bfloat16),
        scratch_shapes=[pltpu.VMEM((-(-rows // SUBLANES) * SUBLANES, width), jnp.float32)],
    )(ticks, prior)


def retiled(blocks):
    groups, depth, width = blocks.shape
    if width % LANES == 0:
        return blocks
    join = TILE // width
    grouped = blocks.reshape(groups // join, join, depth, width)
    return jnp.transpose(grouped, (0, 2, 1, 3)).reshape(groups // join, depth, TILE)


def tree(terms):
    terms = list(terms)
    while len(terms) > 1:
        paired = [terms[k] + terms[k + 1] for k in range(0, len(terms) - 1, 2)]
        terms = paired + terms[len(paired) * 2 :]
    return terms[0]


def magnitudes(lhs, rhs):
    correlation = jnp.dot(lhs, rhs, preferred_element_type=jnp.float32)
    return jnp.abs(correlation.astype(jnp.bfloat16))


def lane_folded(block):
    return tree(block[:, k : k + LANES] for k in range(0, block.shape[1], LANES))


def sublane_folded(block, rows):
    return tree(block[k : k + rows] for k in range(0, block.shape[0], rows))


def add_rows(totals, partial):
    folded = sublane_folded(partial.T, LANES // 4)
    totals[...] = totals[...] + sublane_folded(folded.astype(jnp.float32), SUBLANES)


def add_columns(totals, partials):
    partial = tree(partials).astype(jnp.float32)
    totals[...] = totals[...] + sublane_folded(partial, SUBLANES)


def unit_totals(left, right, row_totals, column_totals, diagonal):
    columns = [[] for _ in range(CHUNK)]
    for u in range(CHUNK):
        lhs, folded = left[u], []
        for o in range(u if diagonal else 0, CHUNK):
            block = magnitudes(lhs, right[o])
            folded.append(lane_folded(block))
            if diagonal and o == u:
                continue
            columns[o].append(sublane_folded(block, 2 * SUBLANES))
            if len(columns[o]) == 2 or u == CHUNK - 1 or (diagonal and u == o - 1):
                add_columns(column_totals.at[o], columns[o])
                columns[o] = []
        add_rows(row_totals.at[u], tree(folded))


def prepare(series, left, right, window):
    halves = []
    shape = (DEPTH, LANES)
    bar = lax.broadcasted_iota(jnp.int32, shape, 0) + STRIDE * window
    held = (bar != UNIT - 1) & (bar != 2 * UNIT - 1)
    for half in range(2):
        values = series[half, STRIDE * window : STRIDE * window + DEPTH]
        mean = jnp.sum(values, axis=0, keepdims=True) * (1.0 / SPAN)
        centred = jnp.where(held, values - mean, 0.0)
        squares = jnp.sum(centred * centred, axis=0, keepdims=True)
        scaled = centred * lax.rsqrt(jnp.maximum(squares, FLOOR_SQUARES))
        halves.append(scaled.astype(jnp.bfloat16))
    high, low = split_parts(jnp.concatenate(halves, axis=1))
    high, low = high.astype(jnp.float8_e4m3fn), low.astype(jnp.float8_e4m3fn)
    right[...] = jnp.concatenate([high, high, low, low], axis=0)
    left[...] = jnp.concatenate([high, low, high, low], axis=0).T


def lay_out(ticks, priors, series):
    bars = WIN_DEV * STRIDE
    total = LEAD + ticks.shape[0] // 2
    for unit in range(series.shape[1] // UNIT):
        first = unit * bars
        early = min(max(LEAD - first, 0), bars)
        late = min(total - first, bars) - early
        for half in range(2):
            for bar in range(early):
                lane = (2 * (first + bar) + half) * LANES
                row = unit * UNIT + bar
                series[half, row : row + 1] = priors[:, lane : lane + LANES]
            row, end = unit * UNIT + early, (unit + 1) * UNIT
            filled = [jnp.zeros((end - row - late, LANES), jnp.float32)]
            if late:
                begin = 2 * (first + early - LEAD) + half
                filled.insert(0, ticks[pl.ds(begin, late, stride=2), :])
            series[half, row:end] = jnp.concatenate(filled, axis=0)


def partner(index, step, size):
    bit, mirrored = 1, index
    while bit < size:
        if step // bit % 2:
            mirrored = mirrored + bit - 2 * bit * (mirrored // bit % 2)
        bit *= 2
    return mirrored


def connect_kernel(
    groups, tick, prior, out, ticks, priors, series, along_block, own, other, left, right,
    totals, sums, back, load_sem, block_send, block_recv, own_send, own_recv,
    next_send, next_recv, back_send, back_recv,
):
    width = 2 * LANES
    blocks = groups // CHUNK
    time, tile = lax.axis_index("tm"), lax.axis_index("asset")
    core = time % 2
    along = (1 + core + tile) % 2
    crosses = along
    next_time, next_tile = cycle_next(time, tile)
    prev_time, prev_tile = time + (1 - along) * (1 - 2 * core), tile + along * (1 - 2 * tile)
    block, place = time // CHUNK, time % CHUNK

    loads = [
        pltpu.make_async_copy(prior, priors, load_sem.at[0]),
        pltpu.make_async_copy(tick, ticks, load_sem.at[1]),
    ]
    for load in loads:
        load.start()
    barrier = pltpu.get_barrier_semaphore()

    def block_at(s):
        return partner(block, s, blocks)

    def place_at(r):
        return partner(place, r, CHUNK)

    peers = [(block_at(s) * CHUNK + place, tile) for s in range(1, blocks)]
    peers += [(block * CHUNK + place_at(r), tile) for r in range(1, CHUNK)]
    peers += [(time, 1 - tile)]
    for peer in peers:
        pl.semaphore_signal(barrier, inc=1, device_id=peer, device_id_type=pl.DeviceIdType.MESH)
    for load in loads:
        load.wait()
    lay_out(ticks, priors, series)
    pl.semaphore_wait(barrier, len(peers))

    reach = own.shape[2]
    block_rows = CHUNK * UNIT

    def remote(source, target, sent, received, device):
        return pltpu.make_async_remote_copy(
            src_ref=source,
            dst_ref=target,
            send_sem=sent,
            recv_sem=received,
            device_id=device,
            device_id_type=pl.DeviceIdType.MESH,
        )

    def part(s, spot):
        if s:
            return along_block.at[s, :, pl.ds(pl.multiple_of(spot * UNIT, UNIT), reach)]
        return series.at[:, pl.ds(pl.multiple_of(block * block_rows + spot * UNIT, UNIT), reach)]

    def block_copy(s):
        first = pl.multiple_of(block_at(s) * block_rows, UNIT)
        return remote(
            series.at[:, pl.ds(first, along_block.shape[2])],
            along_block.at[s],
            block_send.at[s],
            block_recv.at[s],
            (block_at(s) * CHUNK + place, tile),
        )

    def place_copy(s, r):
        index = s * CHUNK + r
        return remote(
            part(s, place_at(r)),
            own.at[index],
            own_send.at[index],
            own_recv.at[index],
            (block * CHUNK + place_at(r), tile),
        )

    def held_part(s, r):
        return own.at[s * CHUNK + r] if r else part(s, place)

    def next_copy(s, r):
        index = s * CHUNK + r
        return remote(
            held_part(s, r),
            other.at[index],
            next_send.at[index],
            next_recv.at[index],
            (next_time, next_tile),
        )

    steps = [(s, r) for s in range(blocks) for r in range(CHUNK)]
    block_copies = {s: block_copy(s) for s in range(1, blocks)}
    place_copies = {(s, r): place_copy(s, r) for s, r in steps if r}
    next_copies = {step: next_copy(*step) for step in steps}

    def relay(s):
        if s:
            block_copies[s].wait_recv()
        for r in reversed(range(1, CHUNK)):
            place_copies[s, r].start()
        next_copies[s, 0].start()

    def pass_on(s):
        for r in range(1, CHUNK):
            place_copies[s, r].wait_recv()
            next_copies[s, r].start()

    def prepare_set(which, s):
        for r in range(CHUNK):
            if which:
                next_copies[s, r].wait_recv()
        for r in range(CHUNK):
            group = s * CHUNK + r
            source = other.at[group] if which else held_part(s, r)
            for window in range(WIN_DEV):
                prepare(source, left.at[which, window, group], right.at[which, window, group], window)

    def chunk_of(ref, which, window, k):
        return ref.at[which, window, pl.ds(k * CHUNK, CHUNK)]

    def unit(window, row_set, row_chunk, column_set, column_chunk, diagonal=False):
        unit_totals(
            chunk_of(left, row_set, window, row_chunk),
            chunk_of(right, column_set, window, column_chunk),
            chunk_of(totals, row_set, window, row_chunk),
            chunk_of(totals, column_set, window, column_chunk),
            diagonal,
        )

    def own_pairs(s):
        for window in range(WIN_DEV):
            for k in range(s):
                unit(window, 0, s, crosses, k)

    def other_pairs(s):
        for window in range(WIN_DEV):
            for k in range(s):
                unit(window, 1 - crosses, k, 1, s)

    def own_closing(s):
        @pl.when(crosses == 0)
        def _():
            for window in range(WIN_DEV):
                unit(window, 0, s, 0, s, True)

    def other_closing(s):
        @pl.when(crosses == 1)
        def _():
            for window in range(WIN_DEV):
                unit(window, 0, s, 1, s)

        @pl.when(crosses == 0)
        def _():
            for window in range(WIN_DEV):
                unit(window, 1, s, 1, s, True)

    for s in range(1, blocks):
        block_copies[s].start()
    relay(0)
    totals[...] = jnp.zeros_like(totals)
    pass_on(0)
    prepare_set(0, 0)
    relay(1)
    own_closing(0)
    prepare_set(1, 0)
    other_closing(0)
    pass_on(1)
    relay(2)
    prepare_set(0, 1)
    own_pairs(1)
    relay(3)
    own_closing(1)
    prepare_set(1, 1)
    other_pairs(1)
    pass_on(2)
    other_closing(1)
    prepare_set(0, 2)
    own_pairs(2)
    pass_on(3)
    own_closing(2)
    prepare_set(1, 2)
    other_pairs(2)
    other_closing(2)
    prepare_set(0, 3)
    own_pairs(3)
    prepare_set(1, 3)
    other_pairs(3)
    other_closing(3)

    sums[...] = jnp.sum(totals[1], axis=2, keepdims=True)
    returned = remote(sums, back, back_send, back_recv, (prev_time, prev_tile))
    returned.start()
    own_closing(3)
    for copy in (*block_copies.values(), *place_copies.values(), *next_copies.values()):
        copy.wait_send()
    mine = jnp.sum(totals[0], axis=2, keepdims=True)
    returned.wait()
    mine = mine + back[...]
    for s, r in steps:
        first = (block_at(s) * CHUNK + place_at(r)) * width
        lanes = pl.ds(pl.multiple_of(first, LANES), width)
        for window in range(WIN_DEV):
            out[window : window + 1, lanes] = mine[window, s * CHUNK + r]


def connected(tick_bars, prior_bars):
    groups = lax.axis_size("tm")
    ticks, prior = tick_bars.reshape(-1, LANES), prior_bars.reshape(1, -1)
    width = 2 * LANES
    blocks = groups // CHUNK
    reach = -(-(WIN_DEV * STRIDE + LEAD) // (WIN_DEV * STRIDE)) * UNIT
    ahead = reach - UNIT
    shared = (groups, 2, reach, LANES)
    vmem, dma, f8 = pltpu.VMEM, pltpu.SemaphoreType.DMA, jnp.float8_e4m3fn
    raw = pl.pallas_call(
        functools.partial(connect_kernel, groups),
        out_shape=vmem((WIN_DEV, groups * width), jnp.float32),
        in_specs=[pl.BlockSpec(memory_space=pl.ANY)] * 2,
        out_specs=pl.BlockSpec(memory_space=vmem),
        scratch_shapes=[
            vmem(ticks.shape, jnp.float32),
            vmem(prior.shape, jnp.float32),
            vmem((2, groups * UNIT + ahead, LANES), jnp.float32),
            vmem((blocks, 2, CHUNK * UNIT + ahead, LANES), jnp.float32),
            vmem(shared, jnp.float32),
            vmem(shared, jnp.float32),
            vmem((2, WIN_DEV, groups, width, 4 * DEPTH), f8),
            vmem((2, WIN_DEV, groups, 4 * DEPTH, width), f8),
            vmem((2, WIN_DEV, groups, SUBLANES, width), jnp.float32),
            vmem((WIN_DEV, groups, 1, width), jnp.float32),
            vmem((WIN_DEV, groups, 1, width), jnp.float32),
            dma((2,)), dma((blocks,)), dma((blocks,)), dma((groups,)), dma((groups,)),
            dma((groups,)), dma((groups,)), dma, dma,
        ],
        compiler_params=pltpu.CompilerParams(
            collective_id=1,
            has_side_effects=True,
            vmem_limit_bytes=60 * 1024 * 1024,
        ),
    )(ticks, prior)
    return raw * (math.sqrt(SPAN) / (ASSETS * PART_SCALE * PART_SCALE))


def shards(tick_bars, prior_bars):
    groups = lax.axis_size("tm")
    if groups == 4 * CHUNK and ASSETS == groups * 4 * LANES:
        return connected(tick_bars, prior_bars)
    own, other = delivered(local_windows(tick_bars, prior_bars))
    own, other = retiled(own), retiled(other)
    core = lax.axis_index("tm") % 2
    crosses = (core == lax.axis_index("asset")).astype(jnp.int32).reshape(1)
    own_part, other_part = pair_totals(crosses, own, other)
    own_part = jnp.transpose(own_part[:, :, 0], (1, 0, 2)).reshape(WIN_DEV, -1)
    other_part = jnp.transpose(other_part[:, :, 0], (1, 0, 2)).reshape(WIN_DEV, -1)
    returned = around(other_part, False)
    return (own_part + returned) * (math.sqrt(SPAN) / (ASSETS * PART_SCALE * PART_SCALE))


def solution(mesh):
    in_specs = (P("asset", "tm", None), P("asset", "tm", None))
    out_specs = P("tm", "asset")
    return jax.shard_map(shards, mesh=mesh, in_specs=in_specs, out_specs=out_specs, check_vma=False)
```

```python
import functools
import math

import jax
import jax.numpy as jnp
from jax import lax
from jax.experimental import pallas as pl
from jax.experimental.pallas import tpu as pltpu
from jax.sharding import PartitionSpec as P

ASSETS = 8192
SPAN = 30
STRIDE = 5
WIN_DEV = 3
LEAD = 25
DEPTH = 32
TILE = 256
LANES = 128
SUBLANES = 8
CHUNK = 4
DIRECT = 2
UNIT = 16
PART_SCALE = 256.0


FLOOR_SQUARES = 1.0


def cycle_next(time, tile):
    core = time % 2
    along = (1 + core + tile) % 2
    return time + along * (1 - 2 * core), tile + (1 - along) * (1 - 2 * tile)


def around(block, forward):
    times, tiles = lax.axis_size("tm"), lax.axis_size("asset")
    route = []
    for time in range(times):
        for tile in range(tiles):
            next_time, next_tile = cycle_next(time, tile)
            hop = (time * tiles + tile, next_time * tiles + next_tile)
            route.append(hop if forward else hop[::-1])
    return lax.ppermute(block, ("tm", "asset"), route)


def window_stack(extended):
    columns = extended.shape[1]
    count = (extended.shape[0] - SPAN) // STRIDE + 1
    groups = extended.reshape(-1, STRIDE, columns)
    stacked = jnp.stack(
        [groups[offset : offset + count] for offset in range(SPAN // STRIDE)], axis=1
    )
    values = stacked.reshape(count, SPAN, columns)
    centred = values - jnp.mean(values, axis=1, keepdims=True)
    squares = jnp.sum(centred * centred, axis=1, keepdims=True)
    scaled = (centred * lax.rsqrt(jnp.maximum(squares, FLOOR_SQUARES))).astype(jnp.bfloat16)
    return jnp.pad(scaled, ((0, 0), (0, DEPTH - SPAN), (0, 0)))


def split_parts(block):
    scaled = block.astype(jnp.float32) * PART_SCALE
    high = scaled.astype(jnp.float8_e4m3fn).astype(jnp.float32)
    return high, scaled - high


def right_parts(block):
    high, low = split_parts(block)
    return jnp.concatenate([high, high, low, low], axis=0).astype(jnp.float8_e4m3fn)


def strip_totals(rows, source, first, count, column_sums, own_first):
    groups, _, width = source.shape
    high, low = split_parts(rows)
    rows_t = jnp.concatenate([high, low, high, low], axis=0).T.astype(jnp.float8_e4m3fn)
    row_partial = jnp.zeros((width, LANES), jnp.float32)
    for offset in range(count):
        group = lax.rem(first + offset, groups)
        magnitude = jnp.abs(jnp.dot(rows_t, source[group], preferred_element_type=jnp.float32))
        for lane in range(0, width, LANES):
            row_partial = row_partial + magnitude[:, lane : lane + LANES]
        if offset or not own_first:
            folded = jnp.sum(magnitude.reshape(width // SUBLANES, SUBLANES, width), axis=0)
            column_sums[group] = column_sums[group] + folded
    return jnp.sum(row_partial.T, axis=0, keepdims=True)


def fill_parts(source, parts):
    def fill(group, carry):
        parts[group] = right_parts(source[group])
        return carry

    lax.fori_loop(0, source.shape[0], fill, 0)


def diagonal(source, out, column_sums, parts):
    groups = source.shape[0]
    half = groups // 2
    fill_parts(source, parts)
    column_sums[...] = jnp.zeros_like(column_sums)

    def step(index, carry):
        out[index, 0] = strip_totals(source[index], parts, index, half + 1, column_sums, True)
        later = index + half
        out[later, 0] = strip_totals(source[later], parts, later, half, column_sums, True)
        return carry

    lax.fori_loop(0, half, step, 0)
    out[:, 0] = out[:, 0] + jnp.sum(column_sums[...], axis=1, keepdims=True)


def totals_kernel(crosses, own, other, own_out, other_out, column_sums, parts):
    groups = own.shape[0]

    @pl.when(crosses[0] == 1)
    def _():
        fill_parts(other, parts)
        column_sums[...] = jnp.zeros_like(column_sums)

        def step(index, carry):
            own_out[index, 0] = strip_totals(own[index], parts, 0, groups, column_sums, False)
            return carry

        lax.fori_loop(0, groups, step, 0)
        other_out[:, 0] = jnp.sum(column_sums[...], axis=1, keepdims=True)

    @pl.when(crosses[0] == 0)
    def _():
        diagonal(own, own_out, column_sums, parts)
        diagonal(other, other_out, column_sums, parts)


def pair_totals(crosses, own, other):
    groups, depth, width = own.shape
    block = pl.BlockSpec((groups, DEPTH, width), lambda w, *_: (0, w, 0))
    line = pl.BlockSpec((groups, 1, 1, width), lambda w, *_: (0, w, 0, 0))
    return pl.pallas_call(
        totals_kernel,
        out_shape=[jax.ShapeDtypeStruct((groups, depth // DEPTH, 1, width), jnp.float32)] * 2,
        grid_spec=pltpu.PrefetchScalarGridSpec(
            num_scalar_prefetch=1,
            grid=(depth // DEPTH,),
            in_specs=[block, block],
            out_specs=[line, line],
            scratch_shapes=[
                pltpu.VMEM((groups, SUBLANES, width), jnp.float32),
                pltpu.VMEM((groups, 4 * DEPTH, width), jnp.float8_e4m3fn),
            ],
        ),
    )(crosses, own, other)


def windows_kernel(tick, prior, out, series):
    width = series.shape[1]
    lead = prior.shape[1] // width
    for row in range(lead):
        series[row : row + 1] = prior[:, row * width : (row + 1) * width]
    for row in range(tick.shape[1] // width):
        series[lead + row : lead + row + 1] = tick[:, row * width : (row + 1) * width]
    for window in range(out.shape[0] * WIN_DEV):
        values = series[window * STRIDE : window * STRIDE + SPAN]
        centred = values - jnp.sum(values, axis=0, keepdims=True) * (1.0 / SPAN)
        squares = jnp.sum(centred * centred, axis=0, keepdims=True)
        scaled = centred * lax.rsqrt(jnp.maximum(squares, FLOOR_SQUARES))
        scaled = jnp.concatenate([scaled, jnp.zeros((DEPTH - SPAN, width), jnp.float32)], axis=0)
        first = window % WIN_DEV * DEPTH
        out[window // WIN_DEV, first : first + DEPTH] = scaled.astype(jnp.bfloat16)


def deliver_kernel(groups, outgoing, own, other, own_send, own_recv, next_send, next_recv, local_sem):
    time = lax.axis_index("tm")
    tile = lax.axis_index("asset")
    next_time, next_tile = cycle_next(time, tile)
    barrier = pltpu.get_barrier_semaphore()
    for step in range(1, groups):
        peer = lax.rem(time + step, groups)
        pl.semaphore_signal(
            barrier, inc=1, device_id=(peer, tile), device_id_type=pl.DeviceIdType.MESH
        )
    pl.semaphore_signal(
        barrier, inc=1, device_id=(time, 1 - tile), device_id_type=pl.DeviceIdType.MESH
    )
    pl.semaphore_wait(barrier, groups)

    def send(step):
        peer = lax.rem(time + step, groups)
        return pltpu.make_async_remote_copy(
            src_ref=outgoing.at[peer],
            dst_ref=own.at[time],
            send_sem=own_send.at[step],
            recv_sem=own_recv.at[step],
            device_id=(peer, tile),
            device_id_type=pl.DeviceIdType.MESH,
        )

    def forward(step):
        source = lax.rem(time - step + groups, groups)
        return pltpu.make_async_remote_copy(
            src_ref=own.at[source],
            dst_ref=other.at[source],
            send_sem=next_send.at[source],
            recv_sem=next_recv.at[source],
            device_id=(next_time, next_tile),
            device_id_type=pl.DeviceIdType.MESH,
        )

    sends = [send(step) for step in range(1, groups)]
    for copy in sends:
        copy.start()
    local = pltpu.make_async_copy(outgoing.at[time], own.at[time], local_sem)
    local.start()
    local.wait()
    forwards = [forward(step) for step in range(groups)]
    forwards[0].start()
    for step in range(1, groups):
        sends[step - 1].wait_recv()
        forwards[step].start()
    for copy in sends:
        copy.wait_send()
    for group in range(groups):
        arrival = pltpu.make_async_remote_copy(
            src_ref=own.at[group],
            dst_ref=other.at[group],
            send_sem=next_send.at[group],
            recv_sem=next_recv.at[group],
            device_id=(next_time, next_tile),
            device_id_type=pl.DeviceIdType.MESH,
        )
        arrival.wait()


def delivered(outgoing):
    groups = outgoing.shape[0]
    vmem = pl.BlockSpec(memory_space=pltpu.VMEM)
    return pl.pallas_call(
        functools.partial(deliver_kernel, groups),
        out_shape=[jax.ShapeDtypeStruct(outgoing.shape, outgoing.dtype)] * 2,
        in_specs=[vmem],
        out_specs=[vmem, vmem],
        scratch_shapes=[pltpu.SemaphoreType.DMA((groups,))] * 4 + [pltpu.SemaphoreType.DMA],
        compiler_params=pltpu.CompilerParams(collective_id=0, has_side_effects=True),
    )(outgoing)


def local_windows(tick_bars, prior_bars):
    groups = lax.axis_size("tm")
    width = ASSETS // (2 * groups)
    ticks, prior = tick_bars.reshape(1, -1), prior_bars.reshape(1, -1)
    if width % LANES:
        series = jnp.concatenate([prior.reshape(-1, width), ticks.reshape(-1, width)], axis=0)
        return window_stack(series).reshape(groups, WIN_DEV * DEPTH, width)
    rows = (ticks.size + prior.size) // width
    return pl.pallas_call(
        windows_kernel,
        out_shape=jax.ShapeDtypeStruct((groups, WIN_DEV * DEPTH, width), jnp.bfloat16),
        scratch_shapes=[pltpu.VMEM((-(-rows // SUBLANES) * SUBLANES, width), jnp.float32)],
    )(ticks, prior)


def retiled(blocks):
    groups, depth, width = blocks.shape
    if width % LANES == 0:
        return blocks
    join = TILE // width
    grouped = blocks.reshape(groups // join, join, depth, width)
    return jnp.transpose(grouped, (0, 2, 1, 3)).reshape(groups // join, depth, TILE)


def tree(terms):
    terms = list(terms)
    while len(terms) > 1:
        paired = [terms[k] + terms[k + 1] for k in range(0, len(terms) - 1, 2)]
        terms = paired + terms[len(paired) * 2 :]
    return terms[0]


def magnitudes(lhs, rhs):
    correlation = jnp.dot(lhs, rhs, preferred_element_type=jnp.float32)
    return jnp.abs(correlation.astype(jnp.bfloat16))


def lane_folded(block):
    return tree(block[:, k : k + LANES] for k in range(0, block.shape[1], LANES))


def sublane_folded(block, rows):
    return tree(block[k : k + rows] for k in range(0, block.shape[0], rows))


def add_rows(totals, partial):
    folded = sublane_folded(partial.T, 2 * SUBLANES)
    totals[...] = totals[...] + sublane_folded(folded.astype(jnp.float32), SUBLANES)


def add_columns(totals, partials):
    partial = tree(partials).astype(jnp.float32)
    totals[...] = totals[...] + sublane_folded(partial, SUBLANES)


def unit_totals(left, right, row_totals, column_totals, diagonal):
    columns = [[] for _ in range(CHUNK)]
    for u in range(CHUNK):
        lhs, folded = left[u], []
        for o in range(u if diagonal else 0, CHUNK):
            block = magnitudes(lhs, right[o])
            folded.append(lane_folded(block))
            if diagonal and o == u:
                continue
            columns[o].append(sublane_folded(block, 2 * SUBLANES))
            if u == (o if diagonal else CHUNK) - 1:
                add_columns(column_totals.at[o], columns[o])
        add_rows(row_totals.at[u], tree(folded))


def prepare(series, left, right, window):
    halves = []
    shape = (DEPTH, LANES)
    bar = lax.broadcasted_iota(jnp.int32, shape, 0) + STRIDE * window
    held = (bar != UNIT - 1) & (bar != 2 * UNIT - 1)
    for half in range(2):
        values = series[half, STRIDE * window : STRIDE * window + DEPTH]
        mean = jnp.sum(values, axis=0, keepdims=True) * (1.0 / SPAN)
        centred = jnp.where(held, values - mean, 0.0)
        squares = jnp.sum(centred * centred, axis=0, keepdims=True)
        scaled = centred * (lax.rsqrt(jnp.maximum(squares, FLOOR_SQUARES)) * PART_SCALE)
        halves.append(scaled.astype(jnp.bfloat16))
    scaled = jnp.concatenate(halves, axis=1)
    high = scaled.astype(jnp.float8_e4m3fn)
    low = (scaled - high.astype(jnp.bfloat16)).astype(jnp.float8_e4m3fn)
    right[...] = jnp.concatenate([high, high, low, low], axis=0)
    left[...] = jnp.concatenate([high, low, high, low], axis=0).T


def lay_out(ticks, priors, series):
    bars = WIN_DEV * STRIDE
    total = LEAD + ticks.shape[0] // 2
    for unit in range(series.shape[1] // UNIT):
        first = unit * bars
        early = min(max(LEAD - first, 0), bars)
        late = min(total - first, bars) - early
        for half in range(2):
            for bar in range(early):
                lane = (2 * (first + bar) + half) * LANES
                row = unit * UNIT + bar
                series[half, row : row + 1] = priors[:, lane : lane + LANES]
            row, end = unit * UNIT + early, (unit + 1) * UNIT
            filled = [jnp.zeros((end - row - late, LANES), jnp.float32)]
            if late:
                begin = 2 * (first + early - LEAD) + half
                filled.insert(0, ticks[pl.ds(begin, late, stride=2), :])
            series[half, row:end] = jnp.concatenate(filled, axis=0)


def partner(index, step, size):
    bit, mirrored = 1, index
    while bit < size:
        if step // bit % 2:
            mirrored = mirrored + bit - 2 * bit * (mirrored // bit % 2)
        bit *= 2
    return mirrored


def connect_kernel(
    groups, tick, prior, out, ticks, priors, series, along_block, own, other, left, right,
    totals, sums, back, load_sem, block_send, block_recv, own_send, own_recv,
    next_send, next_recv, back_send, back_recv,
):
    width = 2 * LANES
    blocks = groups // CHUNK
    time, tile = lax.axis_index("tm"), lax.axis_index("asset")
    core = time % 2
    along = (1 + core + tile) % 2
    crosses = along
    next_time, next_tile = cycle_next(time, tile)
    prev_time, prev_tile = time + (1 - along) * (1 - 2 * core), tile + along * (1 - 2 * tile)
    block, place = time // CHUNK, time % CHUNK

    loads = [
        pltpu.make_async_copy(prior, priors, load_sem.at[0]),
        pltpu.make_async_copy(tick, ticks, load_sem.at[1]),
    ]
    for load in loads:
        load.start()
    barrier = pltpu.get_barrier_semaphore()

    def block_at(s):
        return partner(block, s, blocks)

    def place_at(r):
        return partner(place, r, CHUNK)

    def owner_at(s, r):
        return block_at(s) * CHUNK + place_at(r)

    peers = [(owner_at(s, r), tile) for s in range(DIRECT) for r in range(CHUNK) if s or r]
    peers += [(owner_at(s, 0), tile) for s in range(DIRECT, blocks)]
    peers += [(time, 1 - tile)]
    for peer in peers:
        pl.semaphore_signal(barrier, inc=1, device_id=peer, device_id_type=pl.DeviceIdType.MESH)
    for load in loads:
        load.wait()
    lay_out(ticks, priors, series)
    pl.semaphore_wait(barrier, len(peers))

    reach = own.shape[2]
    block_rows = CHUNK * UNIT

    def remote(source, target, sent, received, device):
        return pltpu.make_async_remote_copy(
            src_ref=source,
            dst_ref=target,
            send_sem=sent,
            recv_sem=received,
            device_id=device,
            device_id_type=pl.DeviceIdType.MESH,
        )

    def rows_of(owner):
        return series.at[:, pl.ds(pl.multiple_of(owner * UNIT, UNIT), reach)]

    def part(s, spot):
        return along_block.at[s, :, pl.ds(pl.multiple_of(spot * UNIT, UNIT), reach)]

    def block_copy(s):
        first = pl.multiple_of(block_at(s) * block_rows, UNIT)
        return remote(
            series.at[:, pl.ds(first, along_block.shape[2])],
            along_block.at[s],
            block_send.at[s],
            block_recv.at[s],
            (owner_at(s, 0), tile),
        )

    def place_copy(s, r):
        index = s * CHUNK + r
        owner = owner_at(s if s < DIRECT else 0, r)
        return remote(
            rows_of(owner) if s < DIRECT else part(s, place_at(r)),
            own.at[index],
            own_send.at[index],
            own_recv.at[index],
            (owner, tile),
        )

    def held_part(s, r):
        if r or 0 < s < DIRECT:
            return own.at[s * CHUNK + r]
        return part(s, place) if s else rows_of(time)

    def next_copy(s, r):
        index = s * CHUNK + r
        return remote(
            held_part(s, r),
            other.at[index],
            next_send.at[index],
            next_recv.at[index],
            (next_time, next_tile),
        )

    steps = [(s, r) for s in range(blocks) for r in range(CHUNK)]
    arrivals = [1, 3, 2] + list(range(4, CHUNK))
    block_copies = {s: block_copy(s) for s in range(DIRECT, blocks)}
    place_copies = {(s, r): place_copy(s, r) for s, r in steps if r or 0 < s < DIRECT}
    next_copies = {step: next_copy(*step) for step in steps}

    def relay(s):
        if s >= DIRECT:
            block_copies[s].wait_recv()
        for r in reversed(range(CHUNK)):
            if (s, r) in place_copies:
                place_copies[s, r].start()
            else:
                next_copies[s, r].start()

    def pass_on(s):
        for r in arrivals if (s, 0) not in place_copies else reversed(range(CHUNK)):
            place_copies[s, r].wait_recv()
            next_copies[s, r].start()

    def prepare_set(which, s):
        for r in range(CHUNK):
            if which:
                next_copies[s, r].wait_recv()
        for r in range(CHUNK):
            group = s * CHUNK + r
            source = other.at[group] if which else held_part(s, r)
            for window in range(WIN_DEV):
                prepare(source, left.at[which, window, group], right.at[which, window, group], window)

    def chunk_of(ref, which, window, k):
        return ref.at[which, window, pl.ds(k * CHUNK, CHUNK)]

    def unit(window, row_set, row_chunk, column_set, column_chunk, diagonal=False):
        unit_totals(
            chunk_of(left, row_set, window, row_chunk),
            chunk_of(right, column_set, window, column_chunk),
            chunk_of(totals, row_set, window, row_chunk),
            chunk_of(totals, column_set, window, column_chunk),
            diagonal,
        )

    def own_pairs(s):
        for window in range(WIN_DEV):
            for k in range(s):
                unit(window, 0, s, crosses, k)

    def other_pairs(s):
        for window in range(WIN_DEV):
            for k in range(s):
                unit(window, 1 - crosses, k, 1, s)

    def own_closing(s):
        @pl.when(crosses == 0)
        def _():
            for window in range(WIN_DEV):
                unit(window, 0, s, 0, s, True)

    def other_closing(s):
        @pl.when(crosses == 1)
        def _():
            for window in range(WIN_DEV):
                unit(window, 0, s, 1, s)

        @pl.when(crosses == 0)
        def _():
            for window in range(WIN_DEV):
                unit(window, 1, s, 1, s, True)

    relay(0)
    relay(1)
    for s in range(DIRECT, blocks):
        block_copies[s].start()
    totals[...] = jnp.zeros_like(totals)
    pass_on(0)
    prepare_set(0, 0)
    own_closing(0)
    prepare_set(1, 0)
    other_closing(0)
    pass_on(1)
    relay(2)
    prepare_set(0, 1)
    own_pairs(1)
    relay(3)
    own_closing(1)
    prepare_set(1, 1)
    other_pairs(1)
    pass_on(2)
    other_closing(1)
    prepare_set(0, 2)
    own_pairs(2)
    pass_on(3)
    own_closing(2)
    prepare_set(1, 2)
    other_pairs(2)
    other_closing(2)
    prepare_set(0, 3)
    own_pairs(3)
    prepare_set(1, 3)
    other_pairs(3)
    other_closing(3)

    sums[...] = jnp.sum(totals[1], axis=2, keepdims=True)
    returned = remote(sums, back, back_send, back_recv, (prev_time, prev_tile))
    returned.start()
    own_closing(3)
    for copy in (*block_copies.values(), *place_copies.values(), *next_copies.values()):
        copy.wait_send()
    mine = jnp.sum(totals[0], axis=2, keepdims=True)
    returned.wait()
    mine = mine + back[...]
    for s, r in steps:
        first = owner_at(s, r) * width
        lanes = pl.ds(pl.multiple_of(first, LANES), width)
        for window in range(WIN_DEV):
            out[window : window + 1, lanes] = mine[window, s * CHUNK + r]


def connected(tick_bars, prior_bars):
    groups = lax.axis_size("tm")
    ticks, prior = tick_bars.reshape(-1, LANES), prior_bars.reshape(1, -1)
    width = 2 * LANES
    blocks = groups // CHUNK
    reach = -(-(WIN_DEV * STRIDE + LEAD) // (WIN_DEV * STRIDE)) * UNIT
    ahead = reach - UNIT
    shared = (groups, 2, reach, LANES)
    vmem, dma, f8 = pltpu.VMEM, pltpu.SemaphoreType.DMA, jnp.float8_e4m3fn
    raw = pl.pallas_call(
        functools.partial(connect_kernel, groups),
        out_shape=vmem((WIN_DEV, groups * width), jnp.float32),
        in_specs=[pl.BlockSpec(memory_space=pl.ANY)] * 2,
        out_specs=pl.BlockSpec(memory_space=vmem),
        scratch_shapes=[
            vmem(ticks.shape, jnp.float32),
            vmem(prior.shape, jnp.float32),
            vmem((2, groups * UNIT + ahead, LANES), jnp.float32),
            vmem((blocks, 2, CHUNK * UNIT + ahead, LANES), jnp.float32),
            vmem(shared, jnp.float32),
            vmem(shared, jnp.float32),
            vmem((2, WIN_DEV, groups, width, 4 * DEPTH), f8),
            vmem((2, WIN_DEV, groups, 4 * DEPTH, width), f8),
            vmem((2, WIN_DEV, groups, SUBLANES, width), jnp.float32),
            vmem((WIN_DEV, groups, 1, width), jnp.float32),
            vmem((WIN_DEV, groups, 1, width), jnp.float32),
            dma((2,)), dma((blocks,)), dma((blocks,)), dma((groups,)), dma((groups,)),
            dma((groups,)), dma((groups,)), dma, dma,
        ],
        compiler_params=pltpu.CompilerParams(
            collective_id=1,
            has_side_effects=True,
            vmem_limit_bytes=60 * 1024 * 1024,
        ),
    )(ticks, prior)
    return raw * (math.sqrt(SPAN) / (ASSETS * PART_SCALE * PART_SCALE))


def shards(tick_bars, prior_bars):
    groups = lax.axis_size("tm")
    if groups == 4 * CHUNK and ASSETS == groups * 4 * LANES:
        return connected(tick_bars, prior_bars)
    own, other = delivered(local_windows(tick_bars, prior_bars))
    own, other = retiled(own), retiled(other)
    core = lax.axis_index("tm") % 2
    crosses = (core == lax.axis_index("asset")).astype(jnp.int32).reshape(1)
    own_part, other_part = pair_totals(crosses, own, other)
    own_part = jnp.transpose(own_part[:, :, 0], (1, 0, 2)).reshape(WIN_DEV, -1)
    other_part = jnp.transpose(other_part[:, :, 0], (1, 0, 2)).reshape(WIN_DEV, -1)
    returned = around(other_part, False)
    return (own_part + returned) * (math.sqrt(SPAN) / (ASSETS * PART_SCALE * PART_SCALE))


def solution(mesh):
    in_specs = (P("asset", "tm", None), P("asset", "tm", None))
    out_specs = P("tm", "asset")
    return jax.shard_map(shards, mesh=mesh, in_specs=in_specs, out_specs=out_specs, check_vma=False)
```

```python
import functools
import math

import jax
import jax.numpy as jnp
from jax import lax
from jax.experimental import pallas as pl
from jax.experimental.pallas import tpu as pltpu
from jax.sharding import PartitionSpec as P

ASSETS = 8192
SPAN = 30
STRIDE = 5
WIN_DEV = 3
LEAD = 25
DEPTH = 32
TILE = 256
LANES = 128
SUBLANES = 8
CHUNK = 4
DIRECT = 2
UNIT = 16
PART_SCALE = 256.0


FLOOR_SQUARES = 1.0


def cycle_next(time, tile):
    core = time % 2
    along = (1 + core + tile) % 2
    return time + along * (1 - 2 * core), tile + (1 - along) * (1 - 2 * tile)


def around(block, forward):
    times, tiles = lax.axis_size("tm"), lax.axis_size("asset")
    route = []
    for time in range(times):
        for tile in range(tiles):
            next_time, next_tile = cycle_next(time, tile)
            hop = (time * tiles + tile, next_time * tiles + next_tile)
            route.append(hop if forward else hop[::-1])
    return lax.ppermute(block, ("tm", "asset"), route)


def window_stack(extended):
    columns = extended.shape[1]
    count = (extended.shape[0] - SPAN) // STRIDE + 1
    groups = extended.reshape(-1, STRIDE, columns)
    stacked = jnp.stack(
        [groups[offset : offset + count] for offset in range(SPAN // STRIDE)], axis=1
    )
    values = stacked.reshape(count, SPAN, columns)
    centred = values - jnp.mean(values, axis=1, keepdims=True)
    squares = jnp.sum(centred * centred, axis=1, keepdims=True)
    scaled = (centred * lax.rsqrt(jnp.maximum(squares, FLOOR_SQUARES))).astype(jnp.bfloat16)
    return jnp.pad(scaled, ((0, 0), (0, DEPTH - SPAN), (0, 0)))


def split_parts(block):
    scaled = block.astype(jnp.float32) * PART_SCALE
    high = scaled.astype(jnp.float8_e4m3fn).astype(jnp.float32)
    return high, scaled - high


def right_parts(block):
    high, low = split_parts(block)
    return jnp.concatenate([high, high, low, low], axis=0).astype(jnp.float8_e4m3fn)


def strip_totals(rows, source, first, count, column_sums, own_first):
    groups, _, width = source.shape
    high, low = split_parts(rows)
    rows_t = jnp.concatenate([high, low, high, low], axis=0).T.astype(jnp.float8_e4m3fn)
    row_partial = jnp.zeros((width, LANES), jnp.float32)
    for offset in range(count):
        group = lax.rem(first + offset, groups)
        magnitude = jnp.abs(jnp.dot(rows_t, source[group], preferred_element_type=jnp.float32))
        for lane in range(0, width, LANES):
            row_partial = row_partial + magnitude[:, lane : lane + LANES]
        if offset or not own_first:
            folded = jnp.sum(magnitude.reshape(width // SUBLANES, SUBLANES, width), axis=0)
            column_sums[group] = column_sums[group] + folded
    return jnp.sum(row_partial.T, axis=0, keepdims=True)


def fill_parts(source, parts):
    def fill(group, carry):
        parts[group] = right_parts(source[group])
        return carry

    lax.fori_loop(0, source.shape[0], fill, 0)


def diagonal(source, out, column_sums, parts):
    groups = source.shape[0]
    half = groups // 2
    fill_parts(source, parts)
    column_sums[...] = jnp.zeros_like(column_sums)

    def step(index, carry):
        out[index, 0] = strip_totals(source[index], parts, index, half + 1, column_sums, True)
        later = index + half
        out[later, 0] = strip_totals(source[later], parts, later, half, column_sums, True)
        return carry

    lax.fori_loop(0, half, step, 0)
    out[:, 0] = out[:, 0] + jnp.sum(column_sums[...], axis=1, keepdims=True)


def totals_kernel(crosses, own, other, own_out, other_out, column_sums, parts):
    groups = own.shape[0]

    @pl.when(crosses[0] == 1)
    def _():
        fill_parts(other, parts)
        column_sums[...] = jnp.zeros_like(column_sums)

        def step(index, carry):
            own_out[index, 0] = strip_totals(own[index], parts, 0, groups, column_sums, False)
            return carry

        lax.fori_loop(0, groups, step, 0)
        other_out[:, 0] = jnp.sum(column_sums[...], axis=1, keepdims=True)

    @pl.when(crosses[0] == 0)
    def _():
        diagonal(own, own_out, column_sums, parts)
        diagonal(other, other_out, column_sums, parts)


def pair_totals(crosses, own, other):
    groups, depth, width = own.shape
    block = pl.BlockSpec((groups, DEPTH, width), lambda w, *_: (0, w, 0))
    line = pl.BlockSpec((groups, 1, 1, width), lambda w, *_: (0, w, 0, 0))
    return pl.pallas_call(
        totals_kernel,
        out_shape=[jax.ShapeDtypeStruct((groups, depth // DEPTH, 1, width), jnp.float32)] * 2,
        grid_spec=pltpu.PrefetchScalarGridSpec(
            num_scalar_prefetch=1,
            grid=(depth // DEPTH,),
            in_specs=[block, block],
            out_specs=[line, line],
            scratch_shapes=[
                pltpu.VMEM((groups, SUBLANES, width), jnp.float32),
                pltpu.VMEM((groups, 4 * DEPTH, width), jnp.float8_e4m3fn),
            ],
        ),
    )(crosses, own, other)


def windows_kernel(tick, prior, out, series):
    width = series.shape[1]
    lead = prior.shape[1] // width
    for row in range(lead):
        series[row : row + 1] = prior[:, row * width : (row + 1) * width]
    for row in range(tick.shape[1] // width):
        series[lead + row : lead + row + 1] = tick[:, row * width : (row + 1) * width]
    for window in range(out.shape[0] * WIN_DEV):
        values = series[window * STRIDE : window * STRIDE + SPAN]
        centred = values - jnp.sum(values, axis=0, keepdims=True) * (1.0 / SPAN)
        squares = jnp.sum(centred * centred, axis=0, keepdims=True)
        scaled = centred * lax.rsqrt(jnp.maximum(squares, FLOOR_SQUARES))
        scaled = jnp.concatenate([scaled, jnp.zeros((DEPTH - SPAN, width), jnp.float32)], axis=0)
        first = window % WIN_DEV * DEPTH
        out[window // WIN_DEV, first : first + DEPTH] = scaled.astype(jnp.bfloat16)


def deliver_kernel(groups, outgoing, own, other, own_send, own_recv, next_send, next_recv, local_sem):
    time = lax.axis_index("tm")
    tile = lax.axis_index("asset")
    next_time, next_tile = cycle_next(time, tile)
    barrier = pltpu.get_barrier_semaphore()
    for step in range(1, groups):
        peer = lax.rem(time + step, groups)
        pl.semaphore_signal(
            barrier, inc=1, device_id=(peer, tile), device_id_type=pl.DeviceIdType.MESH
        )
    pl.semaphore_signal(
        barrier, inc=1, device_id=(time, 1 - tile), device_id_type=pl.DeviceIdType.MESH
    )
    pl.semaphore_wait(barrier, groups)

    def send(step):
        peer = lax.rem(time + step, groups)
        return pltpu.make_async_remote_copy(
            src_ref=outgoing.at[peer],
            dst_ref=own.at[time],
            send_sem=own_send.at[step],
            recv_sem=own_recv.at[step],
            device_id=(peer, tile),
            device_id_type=pl.DeviceIdType.MESH,
        )

    def forward(step):
        source = lax.rem(time - step + groups, groups)
        return pltpu.make_async_remote_copy(
            src_ref=own.at[source],
            dst_ref=other.at[source],
            send_sem=next_send.at[source],
            recv_sem=next_recv.at[source],
            device_id=(next_time, next_tile),
            device_id_type=pl.DeviceIdType.MESH,
        )

    sends = [send(step) for step in range(1, groups)]
    for copy in sends:
        copy.start()
    local = pltpu.make_async_copy(outgoing.at[time], own.at[time], local_sem)
    local.start()
    local.wait()
    forwards = [forward(step) for step in range(groups)]
    forwards[0].start()
    for step in range(1, groups):
        sends[step - 1].wait_recv()
        forwards[step].start()
    for copy in sends:
        copy.wait_send()
    for group in range(groups):
        arrival = pltpu.make_async_remote_copy(
            src_ref=own.at[group],
            dst_ref=other.at[group],
            send_sem=next_send.at[group],
            recv_sem=next_recv.at[group],
            device_id=(next_time, next_tile),
            device_id_type=pl.DeviceIdType.MESH,
        )
        arrival.wait()


def delivered(outgoing):
    groups = outgoing.shape[0]
    vmem = pl.BlockSpec(memory_space=pltpu.VMEM)
    return pl.pallas_call(
        functools.partial(deliver_kernel, groups),
        out_shape=[jax.ShapeDtypeStruct(outgoing.shape, outgoing.dtype)] * 2,
        in_specs=[vmem],
        out_specs=[vmem, vmem],
        scratch_shapes=[pltpu.SemaphoreType.DMA((groups,))] * 4 + [pltpu.SemaphoreType.DMA],
        compiler_params=pltpu.CompilerParams(collective_id=0, has_side_effects=True),
    )(outgoing)


def local_windows(tick_bars, prior_bars):
    groups = lax.axis_size("tm")
    width = ASSETS // (2 * groups)
    ticks, prior = tick_bars.reshape(1, -1), prior_bars.reshape(1, -1)
    if width % LANES:
        series = jnp.concatenate([prior.reshape(-1, width), ticks.reshape(-1, width)], axis=0)
        return window_stack(series).reshape(groups, WIN_DEV * DEPTH, width)
    rows = (ticks.size + prior.size) // width
    return pl.pallas_call(
        windows_kernel,
        out_shape=jax.ShapeDtypeStruct((groups, WIN_DEV * DEPTH, width), jnp.bfloat16),
        scratch_shapes=[pltpu.VMEM((-(-rows // SUBLANES) * SUBLANES, width), jnp.float32)],
    )(ticks, prior)


def retiled(blocks):
    groups, depth, width = blocks.shape
    if width % LANES == 0:
        return blocks
    join = TILE // width
    grouped = blocks.reshape(groups // join, join, depth, width)
    return jnp.transpose(grouped, (0, 2, 1, 3)).reshape(groups // join, depth, TILE)


def tree(terms):
    terms = list(terms)
    while len(terms) > 1:
        paired = [terms[k] + terms[k + 1] for k in range(0, len(terms) - 1, 2)]
        terms = paired + terms[len(paired) * 2 :]
    return terms[0]


def magnitudes(lhs, rhs):
    correlation = jnp.dot(lhs, rhs, preferred_element_type=jnp.float32)
    return jnp.abs(correlation.astype(jnp.bfloat16))


def lane_folded(block):
    return tree(block[:, k : k + LANES] for k in range(0, block.shape[1], LANES))


def sublane_folded(block, rows):
    return tree(block[k : k + rows] for k in range(0, block.shape[0], rows))


def add_rows(totals, partial):
    folded = sublane_folded(partial.T, 2 * SUBLANES)
    totals[...] = totals[...] + sublane_folded(folded.astype(jnp.float32), SUBLANES)


def add_columns(totals, partial):
    totals[...] = totals[...] + sublane_folded(partial.astype(jnp.float32), SUBLANES)


def unit_totals(left, right, row_totals, column_totals, diagonal):
    columns = [None] * CHUNK
    for u in range(CHUNK):
        lhs, first = left[u], u if diagonal else 0
        for o in range(first, CHUNK):
            block = magnitudes(lhs, right[o])
            folded = folded + lane_folded(block) if o > first else lane_folded(block)
            if diagonal and o == u:
                continue
            half = block.shape[0] // 2
            pair = [block[k : k + 2 * SUBLANES] for k in (0, half)]
            for k in range(2 * SUBLANES, half, 2 * SUBLANES):
                pair = [pair[e] + block[e * half + k : e * half + k + 2 * SUBLANES] for e in (0, 1)]
            columns[o] = columns[o] + (pair[0] + pair[1]) if u else pair[0] + pair[1]
            if u == (o if diagonal else CHUNK) - 1:
                add_columns(column_totals.at[o], columns[o])
        add_rows(row_totals.at[u], folded)


def prepare(series, left, right, window):
    halves = []
    shape = (DEPTH, LANES)
    bar = lax.broadcasted_iota(jnp.int32, shape, 0) + STRIDE * window
    held = (bar != UNIT - 1) & (bar != 2 * UNIT - 1)
    for half in range(2):
        values = series[half, STRIDE * window : STRIDE * window + DEPTH]
        mean = jnp.sum(values, axis=0, keepdims=True) * (1.0 / SPAN)
        centred = jnp.where(held, values - mean, 0.0)
        squares = jnp.sum(centred * centred, axis=0, keepdims=True)
        scaled = centred * (lax.rsqrt(jnp.maximum(squares, FLOOR_SQUARES)) * PART_SCALE)
        halves.append(scaled.astype(jnp.bfloat16))
    scaled = jnp.concatenate(halves, axis=1)
    high = scaled.astype(jnp.float8_e4m3fn)
    low = (scaled - high.astype(jnp.bfloat16)).astype(jnp.float8_e4m3fn)
    right[...] = jnp.concatenate([high, high, low, low], axis=0)
    left[...] = jnp.concatenate([high, low, high, low], axis=0).T


def lay_out(ticks, priors, series):
    bars = WIN_DEV * STRIDE
    total = LEAD + ticks.shape[0] // 2
    for unit in range(series.shape[1] // UNIT):
        first = unit * bars
        early = min(max(LEAD - first, 0), bars)
        late = min(total - first, bars) - early
        for half in range(2):
            for bar in range(early):
                lane = (2 * (first + bar) + half) * LANES
                row = unit * UNIT + bar
                series[half, row : row + 1] = priors[:, lane : lane + LANES]
            row, end = unit * UNIT + early, (unit + 1) * UNIT
            filled = [jnp.zeros((end - row - late, LANES), jnp.float32)]
            if late:
                begin = 2 * (first + early - LEAD) + half
                filled.insert(0, ticks[pl.ds(begin, late, stride=2), :])
            series[half, row:end] = jnp.concatenate(filled, axis=0)


def partner(index, step, size):
    bit, mirrored = 1, index
    while bit < size:
        if step // bit % 2:
            mirrored = mirrored + bit - 2 * bit * (mirrored // bit % 2)
        bit *= 2
    return mirrored


def connect_kernel(
    groups, tick, prior, out, ticks, priors, series, along_block, own, other, left, right,
    totals, sums, back, load_sem, block_send, block_recv, own_send, own_recv,
    next_send, next_recv, back_send, back_recv,
):
    width = 2 * LANES
    blocks = groups // CHUNK
    time, tile = lax.axis_index("tm"), lax.axis_index("asset")
    core = time % 2
    along = (1 + core + tile) % 2
    crosses = along
    next_time, next_tile = cycle_next(time, tile)
    prev_time, prev_tile = time + (1 - along) * (1 - 2 * core), tile + along * (1 - 2 * tile)
    block, place = time // CHUNK, time % CHUNK

    loads = [
        pltpu.make_async_copy(prior, priors, load_sem.at[0]),
        pltpu.make_async_copy(tick, ticks, load_sem.at[1]),
    ]
    for load in loads:
        load.start()
    barrier = pltpu.get_barrier_semaphore()

    def block_at(s):
        return partner(block, s, blocks)

    def place_at(r):
        return partner(place, r, CHUNK)

    def owner_at(s, r):
        return block_at(s) * CHUNK + place_at(r)

    peers = [(owner_at(s, r), tile) for s in range(DIRECT) for r in range(CHUNK) if s or r]
    peers += [(owner_at(s, 0), tile) for s in range(DIRECT, blocks)]
    peers += [(time, 1 - tile)]
    for peer in peers:
        pl.semaphore_signal(barrier, inc=1, device_id=peer, device_id_type=pl.DeviceIdType.MESH)
    for load in loads:
        load.wait()
    lay_out(ticks, priors, series)
    pl.semaphore_wait(barrier, len(peers))

    reach = own.shape[2]
    block_rows = CHUNK * UNIT

    def remote(source, target, sent, received, device):
        return pltpu.make_async_remote_copy(
            src_ref=source,
            dst_ref=target,
            send_sem=sent,
            recv_sem=received,
            device_id=device,
            device_id_type=pl.DeviceIdType.MESH,
        )

    def rows_of(owner):
        return series.at[:, pl.ds(pl.multiple_of(owner * UNIT, UNIT), reach)]

    def part(s, spot):
        return along_block.at[s, :, pl.ds(pl.multiple_of(spot * UNIT, UNIT), reach)]

    def block_copy(s):
        first = pl.multiple_of(block_at(s) * block_rows, UNIT)
        return remote(
            series.at[:, pl.ds(first, along_block.shape[2])],
            along_block.at[s],
            block_send.at[s],
            block_recv.at[s],
            (owner_at(s, 0), tile),
        )

    def place_copy(s, r):
        index = s * CHUNK + r
        owner = owner_at(s if s < DIRECT else 0, r)
        return remote(
            rows_of(owner) if s < DIRECT else part(s, place_at(r)),
            own.at[index],
            own_send.at[index],
            own_recv.at[index],
            (owner, tile),
        )

    def held_part(s, r):
        if r or 0 < s < DIRECT:
            return own.at[s * CHUNK + r]
        return part(s, place) if s else rows_of(time)

    def next_copy(s, r):
        index = s * CHUNK + r
        return remote(
            held_part(s, r),
            other.at[index],
            next_send.at[index],
            next_recv.at[index],
            (next_time, next_tile),
        )

    steps = [(s, r) for s in range(blocks) for r in range(CHUNK)]
    arrivals = [1, 3, 2] + list(range(4, CHUNK))
    block_copies = {s: block_copy(s) for s in range(DIRECT, blocks)}
    place_copies = {(s, r): place_copy(s, r) for s, r in steps if r or 0 < s < DIRECT}
    next_copies = {step: next_copy(*step) for step in steps}

    def relay(s):
        if s >= DIRECT:
            block_copies[s].wait_recv()
        for r in reversed(range(CHUNK)):
            if (s, r) in place_copies:
                place_copies[s, r].start()
            else:
                next_copies[s, r].start()

    def pass_on(s):
        for r in arrivals if (s, 0) not in place_copies else reversed(range(CHUNK)):
            place_copies[s, r].wait_recv()
            next_copies[s, r].start()

    def prepare_set(which, s):
        for r in range(CHUNK):
            if which:
                next_copies[s, r].wait_recv()
        for r in range(CHUNK):
            group = s * CHUNK + r
            source = other.at[group] if which else held_part(s, r)
            for window in range(WIN_DEV):
                prepare(source, left.at[which, window, group], right.at[which, window, group], window)

    def chunk_of(ref, which, window, k):
        return ref.at[which, window, pl.ds(k * CHUNK, CHUNK)]

    def unit(window, row_set, row_chunk, column_set, column_chunk, diagonal=False):
        unit_totals(
            chunk_of(left, row_set, window, row_chunk),
            chunk_of(right, column_set, window, column_chunk),
            chunk_of(totals, row_set, window, row_chunk),
            chunk_of(totals, column_set, window, column_chunk),
            diagonal,
        )

    def own_pairs(s):
        for window in range(WIN_DEV):
            for k in range(s):
                unit(window, 0, s, crosses, k)

    def other_pairs(s):
        for window in range(WIN_DEV):
            for k in range(s):
                unit(window, 1 - crosses, k, 1, s)

    def own_closing(s):
        @pl.when(crosses == 0)
        def _():
            for window in range(WIN_DEV):
                unit(window, 0, s, 0, s, True)

    def other_closing(s):
        @pl.when(crosses == 1)
        def _():
            for window in range(WIN_DEV):
                unit(window, 0, s, 1, s)

        @pl.when(crosses == 0)
        def _():
            for window in range(WIN_DEV):
                unit(window, 1, s, 1, s, True)

    relay(0)
    relay(1)
    for s in range(DIRECT, blocks):
        block_copies[s].start()
    totals[...] = jnp.zeros_like(totals)
    pass_on(0)
    prepare_set(0, 0)
    own_closing(0)
    prepare_set(1, 0)
    other_closing(0)
    pass_on(1)
    prepare_set(0, 1)
    own_pairs(1)
    relay(2)
    own_closing(1)
    prepare_set(1, 1)
    other_pairs(1)
    relay(3)
    other_closing(1)
    pass_on(2)
    prepare_set(0, 2)
    own_pairs(2)
    pass_on(3)
    own_closing(2)
    prepare_set(1, 2)
    other_pairs(2)
    other_closing(2)
    prepare_set(0, 3)
    own_pairs(3)
    prepare_set(1, 3)
    other_pairs(3)
    other_closing(3)

    sums[...] = jnp.sum(totals[1], axis=2, keepdims=True)
    returned = remote(sums, back, back_send, back_recv, (prev_time, prev_tile))
    returned.start()
    own_closing(3)
    for copy in (*block_copies.values(), *place_copies.values(), *next_copies.values()):
        copy.wait_send()
    mine = jnp.sum(totals[0], axis=2, keepdims=True)
    returned.wait()
    mine = mine + back[...]
    for s, r in steps:
        first = owner_at(s, r) * width
        lanes = pl.ds(pl.multiple_of(first, LANES), width)
        for window in range(WIN_DEV):
            out[window : window + 1, lanes] = mine[window, s * CHUNK + r]


def connected(tick_bars, prior_bars):
    groups = lax.axis_size("tm")
    ticks, prior = tick_bars.reshape(-1, LANES), prior_bars.reshape(1, -1)
    width = 2 * LANES
    blocks = groups // CHUNK
    reach = -(-(WIN_DEV * STRIDE + LEAD) // (WIN_DEV * STRIDE)) * UNIT
    ahead = reach - UNIT
    shared = (groups, 2, reach, LANES)
    vmem, dma, f8 = pltpu.VMEM, pltpu.SemaphoreType.DMA, jnp.float8_e4m3fn
    raw = pl.pallas_call(
        functools.partial(connect_kernel, groups),
        out_shape=vmem((WIN_DEV, groups * width), jnp.float32),
        in_specs=[pl.BlockSpec(memory_space=pl.ANY)] * 2,
        out_specs=pl.BlockSpec(memory_space=vmem),
        scratch_shapes=[
            vmem(ticks.shape, jnp.float32),
            vmem(prior.shape, jnp.float32),
            vmem((2, groups * UNIT + ahead, LANES), jnp.float32),
            vmem((blocks, 2, CHUNK * UNIT + ahead, LANES), jnp.float32),
            vmem(shared, jnp.float32),
            vmem(shared, jnp.float32),
            vmem((2, WIN_DEV, groups, width, 4 * DEPTH), f8),
            vmem((2, WIN_DEV, groups, 4 * DEPTH, width), f8),
            vmem((2, WIN_DEV, groups, SUBLANES, width), jnp.float32),
            vmem((WIN_DEV, groups, 1, width), jnp.float32),
            vmem((WIN_DEV, groups, 1, width), jnp.float32),
            dma((2,)), dma((blocks,)), dma((blocks,)), dma((groups,)), dma((groups,)),
            dma((groups,)), dma((groups,)), dma, dma,
        ],
        compiler_params=pltpu.CompilerParams(
            collective_id=1,
            has_side_effects=True,
            vmem_limit_bytes=60 * 1024 * 1024,
        ),
    )(ticks, prior)
    return raw * (math.sqrt(SPAN) / (ASSETS * PART_SCALE * PART_SCALE))


def shards(tick_bars, prior_bars):
    groups = lax.axis_size("tm")
    if groups == 4 * CHUNK and ASSETS == groups * 4 * LANES:
        return connected(tick_bars, prior_bars)
    own, other = delivered(local_windows(tick_bars, prior_bars))
    own, other = retiled(own), retiled(other)
    core = lax.axis_index("tm") % 2
    crosses = (core == lax.axis_index("asset")).astype(jnp.int32).reshape(1)
    own_part, other_part = pair_totals(crosses, own, other)
    own_part = jnp.transpose(own_part[:, :, 0], (1, 0, 2)).reshape(WIN_DEV, -1)
    other_part = jnp.transpose(other_part[:, :, 0], (1, 0, 2)).reshape(WIN_DEV, -1)
    returned = around(other_part, False)
    return (own_part + returned) * (math.sqrt(SPAN) / (ASSETS * PART_SCALE * PART_SCALE))


def solution(mesh):
    in_specs = (P("asset", "tm", None), P("asset", "tm", None))
    out_specs = P("tm", "asset")
    return jax.shard_map(shards, mesh=mesh, in_specs=in_specs, out_specs=out_specs, check_vma=False)
```
